16 devices in a mesh: rep: 1, dp: 16 (over x, y, z, core).
Axes of the slice: x: 2, y: 2, z: 2, core: 2. Of those that a mesh axis runs over, the one named last changes fastest.
Arguments:
- x: bfloat16 [16, 2048, 1280], P(('rep', 'dp'))
- dy: bfloat16 [16, 2048, 1280], P(('rep', 'dp'))
- wq: bfloat16 [2, 1280, 1280], P(None, 'dp')
- wk: bfloat16 [2, 1280, 1280], P(None, 'dp')
- wv: bfloat16 [2, 1280, 1280], P(None, 'dp')
- wo: bfloat16 [2, 1280, 1280], P(None, 'dp')
- w_gate: bfloat16 [2, 1280, 3456], P(None, 'dp')
- w_up: bfloat16 [2, 1280, 3456], P(None, 'dp')
- w_down: bfloat16 [2, 3456, 1280], P(None, 'dp')
Outputs:
- output 1: bfloat16 [16, 2048, 1280], P(('rep', 'dp'))
- output 2: bfloat16 [2, 1280, 1280], P('rep', 'dp')
- output 3: bfloat16 [2, 1280, 1280], P('rep', 'dp')
- output 4: bfloat16 [2, 1280, 1280], P('rep', 'dp')
- output 5: bfloat16 [2, 1280, 1280], P('rep', 'dp')
- output 6: bfloat16 [2, 1280, 3456], P('rep', 'dp')
- output 7: bfloat16 [2, 1280, 3456], P('rep', 'dp')
- output 8: bfloat16 [2, 3456, 1280], P('rep', 'dp')
All inputs are finite; a program needn't handle non-finite values.
Results may differ from the reference program's by a relative error of at most 0.0305.
Values are sent between devices in bfloat16 or wider.
A program may use at most 2 GiB of HBM per device.

```python
import jax
import jax.numpy as jnp
from jax import lax

SEQUENCES = 16
TOKENS = 2048
D = 1280
HEADS = 10
KV_HEADS = 10
HEAD = 128
FF = 3456
LAYERS = 2
THETA = 10000
NAMES = ("wq", "wk", "wv", "wo", "w_gate", "w_up", "w_down")
SHAPES = {
    "wq": (LAYERS, D, HEADS * HEAD),
    "wk": (LAYERS, D, KV_HEADS * HEAD),
    "wv": (LAYERS, D, KV_HEADS * HEAD),
    "wo": (LAYERS, HEADS * HEAD, D),
    "w_gate": (LAYERS, D, FF),
    "w_up": (LAYERS, D, FF),
    "w_down": (LAYERS, FF, D),
}


def bump(key, n, height):
    away = (jnp.arange(n, dtype=jnp.int32) - jax.random.randint(key, (), 0, n, jnp.int32)) % n
    return jnp.where(away < n // 8, height, 1.0)


def together(key, own, strength):
    shared = jax.random.normal(key, own.shape[1:], jnp.float32)
    return (own + strength * shared) * lax.rsqrt(1 + strength * strength)


def setup_inputs(seed: int = 0, part: int = 0) -> dict:
    kx, kdy, ka, kb, kz, kf, kh, kl, *keys = jax.random.split(jax.random.key(seed), 8 + 3 * len(NAMES))
    kx, kdy, ka, kb = (jax.random.fold_in(k, part) for k in (kx, kdy, ka, kb))
    kw, km, kv = (keys[i::3] for i in range(3))
    shape = (SEQUENCES, TOKENS, D)
    much_x, much_dy = jax.random.uniform(kz, (2,), jnp.float32, 0.0, 1.0)
    loud = 2.0 ** jax.random.uniform(jax.random.fold_in(kz, 1), (), jnp.float32, -1.0, 2.0)
    layers = 2.0 ** jax.random.uniform(kl, (LAYERS, 1, 1), jnp.float32, -1.0, 1.0)
    times = {"wq": 1.0, "wk": 1.0, "wv": 2.0, "wo": layers, "w_gate": 1.0, "w_up": bump(kh, FF, 4.0), "w_down": layers}
    x = together(ka, jax.random.normal(kx, shape, jnp.float32), much_x) * bump(kf, D, 4.0)
    dy = together(kb, jax.random.normal(kdy, shape, jnp.float32), much_dy)
    drawn = {"x": x.astype(jnp.bfloat16), "dy": (loud * dy * (SEQUENCES * TOKENS) ** -0.5).astype(jnp.bfloat16)}
    for key, name in zip(kw, NAMES, strict=True):
        drawn[name] = (jax.random.normal(key, SHAPES[name], jnp.float32) * SHAPES[name][1] ** -0.5 * times[name]).astype(jnp.bfloat16)
    return drawn


def matmul(a, w):
    return jnp.dot(a, w, preferred_element_type=jnp.float32).astype(jnp.bfloat16)


def normed(h):
    wide = h.astype(jnp.float32)
    scale = lax.rsqrt(jnp.mean(wide**2, -1, keepdims=True) + 1e-6)
    return (wide * scale).astype(jnp.bfloat16)


def turned(t, theta):
    half = t.shape[-1] // 2
    angle = jnp.arange(t.shape[0], dtype=jnp.float32)[:, None] * theta ** (-jnp.arange(half, dtype=jnp.float32) / half)
    cos, sin = jnp.cos(angle)[:, None], jnp.sin(angle)[:, None]
    a, b = t[..., :half].astype(jnp.float32), t[..., half:].astype(jnp.float32)
    return jnp.concatenate([a * cos - b * sin, b * cos + a * sin], -1).astype(jnp.bfloat16)


def seen_by(q, k, v):
    tokens, kv = q.shape[0], k.shape[1]
    q = q.reshape(tokens, kv, -1, q.shape[-1])
    scores = jnp.einsum("tgsd,ugd->gstu", q.astype(jnp.float32), k.astype(jnp.float32)) * q.shape[-1] ** -0.5
    place = jnp.arange(tokens)
    weights = jax.nn.softmax(jnp.where(place[:, None] >= place, scores, -jnp.inf), -1).astype(jnp.bfloat16)
    return jnp.einsum("gstu,ugd->tgsd", weights.astype(jnp.float32), v.astype(jnp.float32)).astype(jnp.bfloat16).reshape(tokens, -1)


def layer(h, w):
    a = normed(h)
    q, k = (turned(matmul(a, w[name]).reshape(h.shape[0], -1, HEAD), THETA) for name in ("wq", "wk"))
    h = h + matmul(seen_by(q, k, matmul(a, w["wv"]).reshape(h.shape[0], -1, HEAD)), w["wo"])
    b = normed(h)
    gate = jnp.dot(b, w["w_gate"], preferred_element_type=jnp.float32)
    up = jnp.dot(b, w["w_up"], preferred_element_type=jnp.float32)
    return h + matmul((jax.nn.silu(gate) * up).astype(jnp.bfloat16), w["w_down"])


def stack(weights, h):
    return lax.scan(lambda h, w: (layer(h, w), None), h, weights)[0]


def reference(x, dy, wq, wk, wv, wo, w_gate, w_up, w_down):
    weights = dict(zip(NAMES, (wq, wk, wv, wo, w_gate, w_up, w_down), strict=True))

    def take(so_far, sequence):
        h, by_y = sequence
        _, back = jax.vjp(stack, weights, h)
        by_weights, by_h = back(by_y)
        return jax.tree.map(lambda total, term: total + term.astype(jnp.float32), so_far, by_weights), by_h

    none_yet = {name: jnp.zeros(w.shape, jnp.float32) for name, w in weights.items()}
    by_weights, by_x = lax.scan(take, none_yet, (x, dy))
    return (by_x, *(by_weights[name].astype(jnp.bfloat16) for name in NAMES))
```

```python
import functools

import jax
import jax.numpy as jnp
from jax import lax
from jax.experimental import pallas as pl
from jax.experimental.pallas import tpu as pltpu
from jax.sharding import PartitionSpec as P

HEAD = 128
THETA = 10000
EPS = 1e-6
LOG2E = 1.4426950408889634
HIDDEN = -2e30
LOW = -1e30
VMEM = 60 * 2**20
BF16, F32 = jnp.bfloat16, jnp.float32


def _dot(a, b, ca, cb):
    return lax.dot_general(a, b, (((ca,), (cb,)), ((), ())), preferred_element_type=F32)


def _call(body, grid, ins, outs, shapes, flops, args, scratch=(), exps=0, once=()):
    specs = [pl.BlockSpec(b, m, pipeline_mode=pl.Buffered(1)) if i in once else pl.BlockSpec(b, m) for i, (b, m) in enumerate(ins)]
    moved = sum(a.size * a.dtype.itemsize for a in (*args, *shapes))
    return pl.pallas_call(
        body,
        grid=grid,
        in_specs=specs,
        out_specs=[pl.BlockSpec(b, m) for b, m in outs],
        out_shape=shapes,
        scratch_shapes=list(scratch),
        compiler_params=pltpu.CompilerParams(vmem_limit_bytes=VMEM, dimension_semantics=("arbitrary",) * len(grid)),
        cost_estimate=pl.CostEstimate(flops=flops, bytes_accessed=moved, transcendentals=exps),
    )(*args)


def _shape(shape, dtype=BF16):
    return jax.ShapeDtypeStruct(shape, dtype)


def _scale(wide):
    return lax.rsqrt(jnp.mean(wide * wide, -1, keepdims=True) + EPS)


def _sum_and_normed(h, part):
    total = (h.astype(F32) + part.astype(BF16).astype(F32)).astype(BF16)
    wide = total.astype(F32)
    return total, (wide * _scale(wide)).astype(BF16)


def _through_norm(h, by_b, by_h):
    wide, c = h.astype(F32), by_b.astype(BF16).astype(F32)
    r = _scale(wide)
    along = jnp.sum(c * wide, -1, keepdims=True)
    part = (c * r - wide * (along * (r * r * r) / wide.shape[-1])).astype(BF16)
    return (by_h.astype(F32) + part.astype(F32)).astype(BF16)


def _turn(t, cos, sin):
    x = t.astype(F32)
    return (x * cos + pltpu.roll(x, HEAD // 2, 1) * sin).astype(BF16)


def _turn_back(t, cos, sin):
    x = t.astype(BF16).astype(F32)
    return (x * cos - pltpu.roll(x, HEAD // 2, 1) * sin).astype(BF16)


def project(a, w, cos, sin):
    (s, d), (n, _, rows, width) = a.shape, w.shape
    bm, sub = min(1024, s), 256

    def body(a_ref, w_ref, c_ref, s_ref, o_ref):
        which, at = pl.program_id(0), pl.program_id(1)
        ww = w_ref[...].reshape(d, width)

        def run(turn):
            for r in range(0, bm, sub):
                t = _dot(a_ref[r : r + sub, :], ww, 1, 0).astype(BF16)
                if turn:
                    here = pl.ds(at * bm + r, sub)
                    c, sn = c_ref[here, :], s_ref[here, :]
                    for x in range(0, width, HEAD):
                        o_ref[0, r : r + sub, x : x + HEAD] = _turn(t[:, x : x + HEAD], c, sn)
                else:
                    o_ref[0, r : r + sub, :] = t

        pl.when(which < 2)(lambda: run(True))
        pl.when(which == 2)(lambda: run(False))

    return _call(
        body, (3, s // bm),
        [((bm, d), lambda m, i: (i, 0)), ((n, 1, rows, width), lambda m, i: (0, m, 0, 0)), ((s, HEAD), lambda m, i: (0, 0)), ((s, HEAD), lambda m, i: (0, 0))],
        [((1, bm, width), lambda m, i: (m, i, 0))], [_shape((3, s, width))], 6 * s * d * width, (a, w, cos, sin), once=(2, 3),
    )[0]


def attend(qkv):
    _, s, width = qkv.shape
    heads = width // HEAD
    hb, b = 5, 512
    e = HEAD**-0.5 * LOG2E

    def body(q_ref, k_ref, v_ref, o_ref, lse_ref, top_s, mix_s):
        iq = pl.program_id(1)
        cols = [slice(i * HEAD, (i + 1) * HEAD) for i in range(hb)]
        top_s[...] = jnp.full(top_s.shape, LOW, F32)
        mix_s[...] = jnp.zeros(mix_s.shape, F32)
        ones = jnp.ones((8, b), BF16)

        def block(j, masked):
            here = pl.ds(pl.multiple_of(j * b, b), b)
            scores = [_dot(k_ref[0, here, c], q_ref[0, :, c], 1, 1) for c in cols]
            if masked:
                seen = lax.broadcasted_iota(jnp.int32, (b, b), 1) >= lax.broadcasted_iota(jnp.int32, (b, b), 0)
            weights, keeps = [], []
            for i, x in enumerate(scores):
                if masked:
                    x = jnp.where(seen, x, HIDDEN)
                old = top_s[i : i + 1, :]
                top = jnp.maximum(old, x.max(axis=0, keepdims=True))
                top_s[i : i + 1, :] = top
                weights.append(jnp.exp2((x - top) * e).astype(BF16))
                keeps.append(jnp.exp2((old - top) * e))
            for i, (c, p, keep) in enumerate(zip(cols, weights, keeps)):
                values = jnp.concatenate([v_ref[0, here, c].T, ones], axis=0)
                mix_s[i] = mix_s[i] * keep + _dot(values, p, 1, 0)

        lax.fori_loop(0, iq, lambda j, _: block(j, False), None)
        block(iq, True)
        for i, c in enumerate(cols):
            total = mix_s[i, HEAD : HEAD + 1, :]
            o_ref[:, c] = (mix_s[i, :HEAD, :] * (1 / total)).T.astype(BF16)
            lse_ref[0, i : i + 1, :] = top_s[i : i + 1, :] * e + jnp.log2(total)

    return _call(
        body, (heads // hb, s // b),
        [((1, b, hb * HEAD), lambda g, i: (0, i, g)), ((1, s, hb * HEAD), lambda g, i: (1, 0, g)), ((1, s, hb * HEAD), lambda g, i: (2, 0, g))],
        [((b, hb * HEAD), lambda g, i: (i, g)), ((1, hb, b), lambda g, i: (g, 0, i))],
        [_shape((s, width)), _shape((heads // hb, hb, s), F32)], 2 * s * s * width, (qkv, qkv, qkv),
        [pltpu.VMEM((hb, b), F32), pltpu.VMEM((hb, HEAD + 8, b), F32)], exps=heads * s * s // 2,
    )


def add_matmul(a, w, h):
    s, d, width = a.shape[0], a.shape[1], h.shape[1]
    bm, sub = 512, 256

    def body(a_ref, w_ref, h_ref, o_ref, b_ref):
        ww = w_ref[...].reshape(d, width)
        for r in range(0, bm, sub):
            here = slice(r, r + sub)
            o_ref[here, :], b_ref[here, :] = _sum_and_normed(h_ref[here, :], _dot(a_ref[here, :], ww, 1, 0))

    zero = (0,) * w.ndim
    row = lambda i: (i, 0)
    return _call(
        body, (s // bm,), [((bm, d), row), (w.shape, lambda i: zero), ((bm, width), row)], [((bm, width), row)] * 2,
        [_shape((s, width))] * 2, 2 * s * d * width, (a, w, h), once=(1,),
    )


def gate_up(b, w):
    (s, d), (n, _, rows, ff) = b.shape, w.shape
    bn, sub = 384, 256

    def body(b_ref, w_ref, g_ref, u_ref, act_ref):
        ww = jnp.concatenate([w_ref[:, 0].reshape(d, bn), w_ref[:, 1].reshape(d, bn)], axis=1)
        for r in range(0, s, sub):
            here = slice(r, r + sub)
            t = _dot(b_ref[here, :], ww, 1, 0)
            g, u = t[:, :bn], t[:, bn:]
            g_ref[here, :] = g
            u_ref[here, :] = u
            act_ref[here, :] = (g * jax.nn.sigmoid(g) * u).astype(BF16)

    col = lambda i: (0, i)
    return _call(
        body, (ff // bn,), [((s, d), lambda i: (0, 0)), ((n, 2, rows, bn), lambda i: (0, 0, 0, i))], [((s, bn), col)] * 3,
        [_shape((s, ff), F32), _shape((s, ff), F32), _shape((s, ff))], 4 * s * d * ff, (b, w), exps=s * ff, once=(0,),
    )


def by_gate_up(by_h, w, g, u):
    (s, d), ff = by_h.shape, w.shape[0]
    bm, step = 256, 768

    def body(y_ref, w_ref, g_ref, u_ref, dg_ref, du_ref):
        y = y_ref[...]
        for x in range(0, ff, step):
            c = slice(x, min(x + step, ff))
            t = _dot(y, w_ref[c, :], 1, 1).astype(BF16).astype(F32)
            gate, up = g_ref[:, c], u_ref[:, c]
            sig = jax.nn.sigmoid(gate)
            part = sig * t
            du_ref[:, c] = (part * gate).astype(BF16)
            dg_ref[:, c] = (part * up * (1 + gate * (1 - sig))).astype(BF16)

    row = lambda i: (i, 0)
    return _call(
        body, (s // bm,), [((bm, d), row), ((ff, d), lambda i: (0, 0)), ((bm, ff), row), ((bm, ff), row)], [((bm, ff), row)] * 2,
        [_shape((s, ff))] * 2, 2 * s * d * ff, (by_h, w, g, u), exps=s * ff, once=(1,),
    )


def back_gate_up(dg, du, w, h, by_h):
    (s, ff), d, n, rows = dg.shape, h.shape[1], w.shape[0], w.shape[2]
    bm = 256

    def body(dg_ref, du_ref, w_ref, h_ref, y_ref, o_ref):
        part = _dot(dg_ref[...], w_ref[:, 0].reshape(d, ff), 1, 1) + _dot(du_ref[...], w_ref[:, 1].reshape(d, ff), 1, 1)
        o_ref[...] = _through_norm(h_ref[...], part, y_ref[...])

    row = lambda i: (i, 0)
    return _call(
        body, (s // bm,), [((bm, ff), row), ((bm, ff), row), (w.shape, lambda i: (0, 0, 0, 0)), ((bm, d), row), ((bm, d), row)], [((bm, d), row)],
        [_shape((s, d))], 4 * s * d * ff, (dg, du, w, h, by_h), once=(2,),
    )[0]


def back_out(by_h, w):
    s, d = by_h.shape
    width = w.shape[0]
    bm = 512

    def body(y_ref, w_ref, o_ref):
        o_ref[...] = _dot(y_ref[...], w_ref[...], 1, 1).astype(BF16)

    row = lambda i: (i, 0)
    return _call(body, (s // bm,), [((bm, d), row), ((width, d), lambda i: (0, 0))], [((bm, width), row)], [_shape((s, width))], 2 * s * d * width, (by_h, w), once=(1,))[0]


def attend_back(qkv, out, lse, by_out, cos, sin):
    _, s, width = qkv.shape
    groups, hb, _ = lse.shape
    b = 512
    scale = HEAD**-0.5
    e = scale * LOG2E

    def body(q_ref, k_ref, v_ref, o_ref, y_ref, lse_ref, c_ref, s_ref, d_ref, dq_s, dk_s, dv_s):
        iq = pl.program_id(1)
        cols = [slice(i * HEAD, (i + 1) * HEAD) for i in range(hb)]

        @pl.when(iq == 0)
        def _():
            dk_s[...] = jnp.zeros_like(dk_s)
            dv_s[...] = jnp.zeros_like(dv_s)

        dq_s[...] = jnp.zeros_like(dq_s)
        deltas = [(y_ref[:, c].astype(F32) * o_ref[:, c].astype(F32)).T.sum(axis=0, keepdims=True) for c in cols]

        def block(j, masked):
            here = pl.ds(pl.multiple_of(j * b, b), b)
            scores = [_dot(k_ref[0, here, c], q_ref[0, :, c], 1, 1) for c in cols]
            dps = [_dot(v_ref[0, here, c], y_ref[:, c], 1, 1) for c in cols]
            if masked:
                seen = lax.broadcasted_iota(jnp.int32, (b, b), 1) >= lax.broadcasted_iota(jnp.int32, (b, b), 0)
            for i, c in enumerate(cols):
                p = jnp.exp2(scores[i] * e - lse_ref[0, i : i + 1, :])
                if masked:
                    p = jnp.where(seen, p, 0.0)
                ds = (p * (dps[i] - deltas[i])).astype(BF16)
                dv_s[i, here, :] += _dot(p.astype(BF16), y_ref[:, c], 1, 0)
                dk_s[i, here, :] += _dot(ds, q_ref[0, :, c], 1, 0)
                dq_s[i] += _dot(k_ref[0, here, c].T, ds, 1, 0)

        lax.fori_loop(0, iq, lambda j, _: block(j, False), None)
        block(iq, True)
        here = pl.ds(pl.multiple_of(iq * b, b), b)
        for i, c in enumerate(cols):
            d_ref[0, here, c] = _turn_back((dq_s[i] * scale).T, c_ref[here, :], s_ref[here, :])

        @pl.when(iq == pl.num_programs(1) - 1)
        def _():
            def finish(j, _):
                rows = pl.ds(pl.multiple_of(j * b, b), b)
                for i, c in enumerate(cols):
                    d_ref[1, rows, c] = _turn_back(dk_s[i, rows, :] * scale, c_ref[rows, :], s_ref[rows, :])
                    d_ref[2, rows, c] = dv_s[i, rows, :].astype(BF16)

            lax.fori_loop(0, s // b, finish, None)

    wide = hb * HEAD
    return _call(
        body, (groups, s // b),
        [((1, b, wide), lambda g, i: (0, i, g)), ((1, s, wide), lambda g, i: (1, 0, g)), ((1, s, wide), lambda g, i: (2, 0, g)),
         ((b, wide), lambda g, i: (i, g)), ((b, wide), lambda g, i: (i, g)), ((1, hb, b), lambda g, i: (g, 0, i)),
         ((s, HEAD), lambda g, i: (0, 0)), ((s, HEAD), lambda g, i: (0, 0))],
        [((3, s, wide), lambda g, i: (0, 0, g))], [_shape((3, s, width))], 5 * s * s * width, (qkv, qkv, qkv, out, by_out, lse, cos, sin),
        [pltpu.VMEM((hb, HEAD, b), F32), pltpu.VMEM((hb, s, HEAD), F32), pltpu.VMEM((hb, s, HEAD), F32)], exps=s * s * width // HEAD // 2, once=(1, 2, 6, 7),
    )[0]


def back_project(d, w, h, by_h):
    (_, s, width), n, rows = d.shape, w.shape[0], w.shape[2]
    dim = h.shape[1]
    bm = 256

    def body(d_ref, w_ref, h_ref, y_ref, o_ref):
        part = sum(_dot(d_ref[m], w_ref[:, m].reshape(dim, width), 1, 1) for m in range(3))
        o_ref[...] = _through_norm(h_ref[...], part, y_ref[...])

    row = lambda i: (i, 0)
    return _call(
        body, (s // bm,), [((3, bm, width), lambda i: (0, i, 0)), ((n, 3, rows, width), lambda i: (0, 0, 0, 0)), ((bm, dim), row), ((bm, dim), row)],
        [((bm, dim), row)], [_shape((s, dim))], 6 * s * dim * width, (d, w, h, by_h), once=(1,),
    )[0]


def grad_project(a, d, n):
    (s, dim), width = a.shape, d.shape[2]
    rows, bn = dim // n, 256

    def body(a_ref, d_ref, o_ref):
        o_ref[:, 0] = _dot(a_ref[...], d_ref[0], 0, 0).astype(BF16).reshape(n, rows, bn)

    return _call(
        body, (3, width // bn), [((s, dim), lambda m, i: (0, 0)), ((1, s, bn), lambda m, i: (m, 0, i))], [((n, 1, rows, bn), lambda m, i: (0, m, 0, i))],
        [_shape((n, 3, rows, width))], 6 * s * dim * width, (a, d), once=(0,),
    )[0]


def grad_gate_up(b, dg, du, n):
    (s, d), ff = b.shape, dg.shape[1]
    rows, bn, third = d // n, 384, ff // 3
    per = third // bn

    def body(b_ref, dg_ref, du_ref, o_ref):
        both = jnp.concatenate([dg_ref[...], du_ref[...]], axis=1)
        for x in range(0, n, 8):
            t = _dot(b_ref[:, x * rows : (x + 8) * rows], both, 0, 0).astype(BF16)
            o_ref[x : x + 8, 0, 0] = t[:, :bn].reshape(8, rows, bn)
            o_ref[x : x + 8, 0, 1] = t[:, bn:].reshape(8, rows, bn)

    col = lambda i: (0, i)
    return _call(
        body, (ff // bn,), [((s, d), lambda i: (0, 0)), ((s, bn), col), ((s, bn), col)],
        [((n, 1, 2, rows, bn), lambda i: (0, i // per, 0, 0, i % per))], [_shape((n, 3, 2, rows, third))], 4 * s * d * ff, (b, dg, du), once=(0,),
    )[0]


def grad_down_out(act, by_h, out, by_mid, n):
    (s, ff), d, width = act.shape, by_h.shape[1], out.shape[1]
    fr, wr, bn = ff // n, width // n, 256
    rows = -(-(fr + wr) // 24) * 24

    def body(act_ref, y_ref, out_ref, m_ref, o_ref):
        y = y_ref[...]
        t = jnp.concatenate([_dot(act_ref[:, x : x + 384], y, 0, 0) for x in range(0, ff, 384)], axis=0)
        for i in range(n):
            o_ref[i, :fr, :] = t[i * fr : (i + 1) * fr, :].astype(BF16)
        t = _dot(out_ref[...], m_ref[...], 0, 0)
        for i in range(n):
            o_ref[i, fr : fr + wr, :] = t[i * wr : (i + 1) * wr, :].astype(BF16)
            o_ref[i, fr + wr :, :] = jnp.zeros((rows - fr - wr, bn), BF16)

    col = lambda i: (0, i)
    return _call(
        body, (d // bn,), [((s, ff), lambda i: (0, 0)), ((s, bn), col), ((s, width), lambda i: (0, 0)), ((s, bn), col)], [((n, rows, bn), lambda i: (0, 0, i))],
        [_shape((n, rows, d))], 2 * s * d * (ff + width), (act, by_h, out, by_mid), once=(0, 2),
    )[0]


def solution(mesh):
    n = mesh.shape["dp"]

    def gather(t):
        return lax.all_gather(t, "dp", axis=0, tiled=True)

    def scatter(t):
        flat = lax.psum_scatter(t.reshape(-1, t.shape[-1]), "dp", scatter_dimension=0, tiled=True)
        return flat.reshape(t.shape[1:])

    def step(x, dy, wq, wk, wv, wo, w_gate, w_up, w_down):
        layers, rows, width = wq.shape
        ff = w_gate.shape[2]
        s = x.shape[1]
        half = HEAD // 2
        angle = jnp.arange(s, dtype=F32)[:, None] * THETA ** (-jnp.arange(half, dtype=F32) / half)
        c, sn = jnp.cos(angle), jnp.sin(angle)
        cos, sin = jnp.concatenate([c, c], -1), jnp.concatenate([-sn, sn], -1)

        h = x[0]
        wide = h.astype(F32)
        a = (wide * _scale(wide)).astype(BF16)
        kept = []
        for l in range(layers):
            w_qkv = gather(jnp.concatenate([wq[l], wk[l], wv[l]], axis=0)).reshape(n, 3, rows, width)
            w_out = gather(wo[l])
            w_gu = gather(jnp.concatenate([w_gate[l], w_up[l]], axis=0)).reshape(n, 2, rows, ff)
            w_dn = gather(w_down[l])
            qkv = project(a, w_qkv, cos, sin)
            out, lse = attend(qkv)
            mid, b = add_matmul(out, w_out, h)
            g, u, act = gate_up(b, w_gu)
            kept.append((w_qkv, w_out, w_gu, w_dn, h, a, qkv, out, lse, mid, b, g, u, act))
            if l + 1 < layers:
                h, a = add_matmul(act, w_dn, mid)

        y = dy[0]
        grads = []
        for l in reversed(range(layers)):
            w_qkv, w_out, w_gu, w_dn, h, a, qkv, out, lse, mid, b, g, u, act = kept[l]
            dg, du = by_gate_up(y, w_dn, g, u)
            of_gu = scatter(grad_gate_up(b, dg, du, n))
            y_mid = back_gate_up(dg, du, w_gu, mid, y)
            of_dn_out = scatter(grad_down_out(act, y, out, y_mid, n))
            d = attend_back(qkv, out, lse, back_out(y_mid, w_out), cos, sin)
            of_qkv = scatter(grad_project(a, d, n))
            y = back_project(d, w_qkv, h, y_mid)
            fr = w_down.shape[1]
            grads.append((of_qkv[0], of_qkv[1], of_qkv[2], of_dn_out[fr : fr + rows], *(jnp.concatenate(list(of_gu[:, i]), axis=-1) for i in (0, 1)), of_dn_out[:fr]))
        grads.reverse()
        return (y[None], *(jnp.stack([g[i] for g in grads]) for i in range(7)))

    states, cut = P(("rep", "dp"), None, None), P(None, "dp", None)
    return jax.shard_map(
        step,
        mesh=mesh,
        in_specs=(states, states) + (cut,) * 7,
        out_specs=(states,) + (P("rep", "dp", None),) * 7,
        check_vma=False,
    )
```

```python
import functools

import jax
import jax.numpy as jnp
import numpy as np
from jax import lax
from jax.experimental import pallas as pl
from jax.experimental.pallas import tpu as pltpu
from jax.sharding import PartitionSpec as P


HEAD = 128
THETA = 10000
EPS = 1e-6
LOG2E = 1.4426950408889634
HIDDEN = -2e30
LOW = -1e30
VMEM = 60 * 2**20
BF16, F32 = jnp.bfloat16, jnp.float32


def _dot(a, b, ca, cb):
    return lax.dot_general(a, b, (((ca,), (cb,)), ((), ())), preferred_element_type=F32)


def _nn(a, b):
    return _dot(a, b, 1, 0)


def _nt(a, b):
    return _dot(a, b, 1, 1)


def _tn(a, b):
    return _dot(a, b, 0, 0)


def _row(i):
    return i, 0


def _col(i):
    return 0, i


class _fixed:
    def __init__(self, rank, *last):
        self.place = (0,) * (rank - len(last)) + last

    def __call__(self, *_):
        return self.place


def _spec(block, index):
    return pl.BlockSpec(block, index, pipeline_mode=pl.Buffered(1)) if isinstance(index, _fixed) else pl.BlockSpec(block, index)


def _step():
    return pl.program_id(0)


def _cuts(size, step):
    return [slice(x, min(x + step, size)) for x in range(0, size, step)]


def _loop(count, body):
    lax.fori_loop(0, count, lambda i, _: body(i), None)


_FLAT, _CUBE, _QUAD = _fixed(2), _fixed(3), _fixed(4)


def _call(body, grid, ins, outs, shapes, work, args, scratch=()):
    moved = sum(a.size * a.dtype.itemsize for a in (*args, *shapes))
    results = pl.pallas_call(
        body,
        grid=grid,
        in_specs=[_spec(*x) for x in ins],
        out_specs=[_spec(*x) for x in outs],
        out_shape=shapes,
        scratch_shapes=list(scratch),
        compiler_params=pltpu.CompilerParams(vmem_limit_bytes=VMEM, dimension_semantics=("arbitrary",) * len(grid)),
        cost_estimate=pl.CostEstimate(flops=2 * work, bytes_accessed=moved, transcendentals=0),
    )(*args)
    return results if len(shapes) > 1 else results[0]


def _shape(shape, dtype=BF16):
    return jax.ShapeDtypeStruct(shape, dtype)


def _scale(wide):
    return lax.rsqrt(jnp.mean(wide * wide, -1, keepdims=True) + EPS)


def _sum_and_normed(h, part):
    total = (h.astype(F32) + part.astype(BF16).astype(F32)).astype(BF16)
    wide = total.astype(F32)
    return total, (wide * _scale(wide)).astype(BF16)


def _through_norm(h, by_b, by_h):
    wide, c = h.astype(F32), by_b.astype(BF16).astype(F32)
    r = _scale(wide)
    along = jnp.sum(c * wide, -1, keepdims=True)
    part = (c * r - wide * (along * (r * r * r) / wide.shape[-1])).astype(BF16)
    return (by_h.astype(F32) + part.astype(F32)).astype(BF16)


def _turn(t, cos, sin):
    x = t.astype(F32)
    return (x * cos + pltpu.roll(x, HEAD // 2, 1) * sin).astype(BF16)


def _turn_back(t, cos, sin):
    x = t.astype(BF16).astype(F32)
    return (x * cos - pltpu.roll(x, HEAD // 2, 1) * sin).astype(BF16)


PARTS = (slice(0, 384), slice(384, 768), slice(768, 1280))
ANY = pl.BlockSpec(memory_space=pl.ANY)
TORUS = (2, 2, 2, 2)
WAYS = range(3)
ALL = slice(None)


def _here():
    me = lax.axis_index("dp")
    bits = [me // 8, me // 4 % 2, me // 2 % 2]
    core = me % 2
    return bits, core, me + 1 - 2 * core, [me + far * (1 - 2 * b) for far, b in zip((8, 4, 2), bits)]


def _order(wave, k):
    return [(k + wave + i) % 3 for i in WAYS]


def _send(source, target, sent, came, device):
    return pltpu.make_async_remote_copy(
        src_ref=source, dst_ref=target, send_sem=sent, recv_sem=came, device_id={"dp": device}, device_id_type=pl.DeviceIdType.MESH
    )


def _meet(devices):
    barrier = pltpu.get_barrier_semaphore()
    for device in devices:
        pl.semaphore_signal(barrier, inc=1, device_id={"dp": device}, device_id_type=pl.DeviceIdType.MESH)
    pl.semaphore_wait(barrier, len(devices))


def _link_sems(waves):
    return [pltpu.SemaphoreType.DMA((waves, 3, 3))] * 2 + [pltpu.SemaphoreType.DMA((waves,))] * 2


class _Spread:
    def __init__(self, own, whole, pick, sems):
        self.own, self.whole, self.pick = own, whole, pick
        self.sent, self.came, self.core_sent, self.core_came, self.stored = sems
        self.bits, self.core, self.other, self.across = _here()

    def _hop(self, wave, stage, k):
        dims = _order(wave, k)
        place = [ALL if i in dims[:stage] else b for i, b in enumerate(self.bits)]
        target = self.whole.at[(*place, self.core, *self.pick[wave], PARTS[k])]
        source = target if stage else self.own.at[(*self.pick[wave], PARTS[k])]
        return _send(source, target, self.sent.at[wave, stage, k], self.came.at[wave, stage, k], self.across[dims[stage]])

    def _to_core(self, wave):
        mine = self.whole.at[(*[ALL] * 3, self.core, *self.pick[wave])]
        return _send(mine, mine, self.core_sent.at[wave], self.core_came.at[wave], self.other)

    def _store(self, wave):
        return pltpu.make_async_copy(self.own.at[self.pick[wave]], self.whole.at[(*self.bits, self.core, *self.pick[wave])], self.stored.at[wave])

    def start(self, wave, stage=0):
        for k in WAYS:
            if stage:
                self._hop(wave, stage - 1, k).wait_recv()
        if stage == 1:
            self._store(wave).wait()
        for k in WAYS:
            if stage < 3:
                self._hop(wave, stage, k).start()
        if stage == 0:
            self._store(wave).start()
        if stage == 3:
            self._to_core(wave).start()

    def finish(self, wave):
        self._to_core(wave).wait()
        for stage in WAYS:
            for k in WAYS:
                self._hop(wave, stage, k).wait_send()


def fetch_and_project(x, cos, sin, *shards):
    (s, d), (_, rows, width) = x.shape, shards[0].shape
    n, waves, bm, sub = 16, len(shards), s // 2, 256

    def body(x_hbm, c_ref, s_ref, *rest):
        parts, (a_ref, o_ref, whole, own_s, x_s, w_s, own_sem, x_sem, w_sem), sems = rest[:waves], rest[waves:-5], rest[-5:]
        t = _step()
        spread = _Spread(own_s, whole, [(i, ALL) for i in range(waves)], sems)

        def own(i):
            return pltpu.make_async_copy(parts[i].at[0], own_s.at[i], own_sem.at[i])

        def states():
            return pltpu.make_async_copy(x_hbm, x_s, x_sem)

        def weights(i):
            return pltpu.make_async_copy(whole.at[(*[ALL] * len(TORUS), i)], w_s.at[i % 2], w_sem)

        def ready(i):
            spread.finish(i)
            weights(i).start()
            weights(i).wait()

        def begin():
            for i in range(waves):
                own(i).start()
            states().start()
            _meet((spread.other, *spread.across))
            for i in range(waves):
                own(i).wait()
                spread.start(i)
            states().wait()

            def norm(i):
                here = pl.ds(pl.multiple_of(i * sub, sub), sub)
                wide = x_s[here, :].astype(F32)
                a_ref[here, :] = (wide * _scale(wide)).astype(BF16)

            _loop(s // sub, norm)
            spread.start(0, 1)
            spread.start(1, 1)
            spread.start(0, 2)
            spread.start(2, 1)
            spread.start(1, 2)
            spread.start(0, 3)
            ready(0)

        pl.when(t == 0)(begin)

        def run(turn, matrix, half):
            ww = w_s[matrix % 2].reshape(d, width)
            for r in range(0, bm, sub):
                here = pl.ds(pl.multiple_of(half * bm + r, sub), sub)
                y = _nn(a_ref[here, :], ww).astype(BF16)
                if turn:
                    c, sn = c_ref[here, :], s_ref[here, :]
                    for k in range(0, width, HEAD):
                        o_ref[0, r : r + sub, k : k + HEAD] = _turn(y[:, k : k + HEAD], c, sn)
                else:
                    o_ref[0, r : r + sub, :] = y

        matrix, half = (t - 1) // 2, (t + 1) % 2
        pl.when((t > 0) & (matrix < 2))(lambda: run(True, matrix, half))
        pl.when(matrix == 2)(lambda: run(False, matrix, half))
        after_step = (), ((spread.start, 2, 2), (spread.start, 1, 3)), ((ready, 1),), ((spread.start, 2, 3),), ((ready, 2),)
        for step, actions in enumerate(after_step):

            @pl.when(t == step)
            def _():
                for action, *args in actions:
                    action(*args)

    def at(t):
        return jnp.maximum(t - 1, 0)

    a, qkv, whole = pl.pallas_call(
        body,
        grid=(7,),
        in_specs=[ANY, *[_spec((s, HEAD), _FLAT)] * 2, *[ANY] * waves],
        out_specs=[pl.BlockSpec((s, d), _FLAT), pl.BlockSpec((1, bm, width), lambda t: (at(t) // 2, at(t) % 2, 0)), ANY],
        out_shape=[_shape((s, d)), _shape((3, s, width)), _shape((*TORUS, waves, rows, width))],
        scratch_shapes=[
            pltpu.VMEM((waves, rows, width), BF16), pltpu.VMEM((s, d), BF16), pltpu.VMEM((2, *TORUS, rows, width), BF16),
            pltpu.SemaphoreType.DMA((waves,)), pltpu.SemaphoreType.DMA, pltpu.SemaphoreType.DMA, *_link_sems(waves), pltpu.SemaphoreType.DMA((waves,)),
        ],
        compiler_params=pltpu.CompilerParams(vmem_limit_bytes=VMEM, collective_id=1, has_side_effects=True),
        cost_estimate=pl.CostEstimate(flops=12 * s * d * width, bytes_accessed=VMEM, transcendentals=0),
    )(x, cos, sin, *shards)
    return a, qkv, whole.reshape(n, waves, rows, width)


def project(a, w, cos, sin):
    (s, d), (n, _, rows, width) = a.shape, w.shape
    bm, sub = min(1024, s), 256

    def body(a_ref, w_ref, c_ref, s_ref, o_ref):
        which, at = _step(), pl.program_id(1)
        ww = w_ref[:].reshape(d, width)

        def run(turn):
            for r in range(0, bm, sub):
                t = _nn(a_ref[r : r + sub, :], ww).astype(BF16)
                if turn:
                    here = pl.ds(at * bm + r, sub)
                    c, sn = c_ref[here, :], s_ref[here, :]
                    for x in range(0, width, HEAD):
                        o_ref[0, r : r + sub, x : x + HEAD] = _turn(t[:, x : x + HEAD], c, sn)
                else:
                    o_ref[0, r : r + sub, :] = t

        pl.when(which < 2)(lambda: run(True))
        pl.when(which == 2)(lambda: run(False))

    return _call(
        body, (3, s // bm),
        [((bm, d), lambda m, i: (i, 0)), ((n, 1, rows, width), lambda m, i: (0, m, 0, 0)), ((s, HEAD), _FLAT), ((s, HEAD), _FLAT)],
        [((1, bm, width), lambda m, i: (m, i, 0))], [_shape((3, s, width))], 3 * s * d * width, (a, w, cos, sin),
    )


def _heads(b, s, hb):
    return [((1, b, hb * HEAD), lambda g, i: (0, i, g)), *(((1, s, hb * HEAD), lambda g, i, m=m: (m, 0, g)) for m in (1, 2))]


def _few(b, hb):
    return (b, hb * HEAD), lambda g, i: (i, g)


def _stats(b, hb):
    return (1, hb, b), lambda g, i: (g, 0, i)


def attend(qkv):
    _, s, width = qkv.shape
    heads = width // HEAD
    hb, b = 5, 512
    e = HEAD**-0.5 * LOG2E

    def body(q_ref, k_ref, v_ref, o_ref, lse_ref, top_s, mix_s):
        iq = pl.program_id(1)
        cols = [slice(i * HEAD, (i + 1) * HEAD) for i in range(hb)]
        top_s[:] = jnp.full(top_s.shape, LOW, F32)
        mix_s[:] = jnp.zeros(mix_s.shape, F32)
        ones = jnp.ones((8, b), BF16)

        def block(j, masked):
            here = pl.ds(pl.multiple_of(j * b, b), b)
            scores = [_nt(k_ref[0, here, c], q_ref[0, :, c]) for c in cols]
            if masked:
                seen = lax.broadcasted_iota(jnp.int32, (b, b), 1) >= lax.broadcasted_iota(jnp.int32, (b, b), 0)
            weights, keeps = [], []
            for i, x in enumerate(scores):
                if masked:
                    x = jnp.where(seen, x, HIDDEN)
                old = top_s[i : i + 1, :]
                top = jnp.maximum(old, x.max(axis=0, keepdims=True))
                top_s[i : i + 1, :] = top
                weights.append(jnp.exp2((x - top) * e).astype(BF16))
                keeps.append(jnp.exp2((old - top) * e))
            for i, (c, p, keep) in enumerate(zip(cols, weights, keeps)):
                values = jnp.concatenate([v_ref[0, here, c].T, ones], axis=0)
                mix_s[i] = mix_s[i] * keep + _nn(values, p)

        _loop(iq, lambda j: block(j, False))
        block(iq, True)
        for i, c in enumerate(cols):
            total = mix_s[i, HEAD : HEAD + 1, :]
            o_ref[:, c] = (mix_s[i, :HEAD, :] * (1 / total)).T.astype(BF16)
            lse_ref[0, i : i + 1, :] = top_s[i : i + 1, :] * e + jnp.log2(total)

    return _call(
        body, (heads // hb, s // b),
        _heads(b, s, hb),
        [_few(b, hb), _stats(b, hb)],
        [_shape((s, width)), _shape((heads // hb, hb, s), F32)], s * s * width, (qkv, qkv, qkv),
        [pltpu.VMEM((hb, b), F32), pltpu.VMEM((hb, HEAD + 8, b), F32)],
    )


def add_matmul(a, w, h, block=None, at=None):
    s, d, width = a.shape[0], a.shape[1], h.shape[1]
    bm, sub = 512, 256
    block, at = block or w.shape, at or (0,) * w.ndim

    def body(a_ref, w_ref, h_ref, o_ref, b_ref):
        ww = w_ref[:].reshape(d, width)
        for here in _cuts(bm, sub):
            o_ref[here, :], b_ref[here, :] = _sum_and_normed(h_ref[here, :], _nn(a_ref[here, :], ww))

    return _call(
        body, (s // bm,), [((bm, d), _row), (block, _fixed(len(at), *at)), ((bm, width), _row)], [((bm, width), _row)] * 2,
        [_shape((s, width))] * 2, s * d * width, (a, w, h),
    )


def gate_up(b, w, shard=None):
    (s, d), (n, _, rows, ff) = b.shape, w.shape
    bn, sub = 384, 256
    steps = ff // bn

    def body(b_ref, w_ref, *rest):
        g_ref, u_ref, act_ref = rest[:3] if shard is None else rest[1:4]
        ww = jnp.concatenate([w_ref[:, 0].reshape(d, bn), w_ref[:, 1].reshape(d, bn)], axis=1)
        for here in _cuts(s, sub):
            t = _nn(b_ref[here, :], ww)
            g, u = t[:, :bn], t[:, bn:]
            g_ref[here, :] = g
            u_ref[here, :] = u
            act_ref[here, :] = (g * jax.nn.sigmoid(g) * u).astype(BF16)

    out_specs, out_shape = [pl.BlockSpec((s, bn), _col)] * 3, [_shape((s, ff), F32), _shape((s, ff), F32), _shape((s, ff))]
    if shard is None:
        return _call(
            body, (steps,), [((s, d), _FLAT), ((n, 2, rows, bn), lambda i: (0, 0, 0, i))], [((s, bn), _col)] * 3,
            out_shape, 2 * s * d * ff, (b, w),
        )
    depth, width = shard.shape
    cut = depth // 16 * 8

    def both(b_ref, w_ref, shard_ref, g_ref, u_ref, act_ref, whole, own_s, own_sem, *sems):
        t = _step()
        spread = _Spread(own_s, whole, [(slice(0, cut),), (slice(cut, depth),)], sems)

        @pl.when(t == 0)
        def _():
            own = pltpu.make_async_copy(shard_ref, own_s, own_sem)
            own.start()
            _meet((spread.other, *spread.across))
            own.wait()
            spread.start(0)
            spread.start(1)

        body(b_ref, w_ref, shard_ref, g_ref, u_ref, act_ref)
        for wave, times in enumerate(((0, 2, 5), (1, 3, 7))):
            for stage, step in enumerate(times):

                @pl.when(t == step)
                def _():
                    spread.start(wave, stage + 1)

        @pl.when(t == steps - 1)
        def _():
            spread.finish(0)
            spread.finish(1)

    *results, whole = pl.pallas_call(
        both,
        grid=(steps,),
        in_specs=[_spec((s, d), _FLAT), pl.BlockSpec((n, 2, rows, bn), lambda i: (0, 0, 0, i)), ANY],
        out_specs=[*out_specs, ANY],
        out_shape=[*out_shape, _shape((*TORUS, depth, width))],
        scratch_shapes=[pltpu.VMEM((depth, width), BF16), pltpu.SemaphoreType.DMA, *_link_sems(2), pltpu.SemaphoreType.DMA((2,))],
        compiler_params=pltpu.CompilerParams(vmem_limit_bytes=VMEM, collective_id=2, has_side_effects=True),
        cost_estimate=pl.CostEstimate(flops=2 * s * d * ff, bytes_accessed=VMEM, transcendentals=s * ff),
    )(b, w, shard)
    return *results, whole.reshape(n * depth, width)


def back_gate_up(dg, du, w, h, by_h):
    (s, ff), d = dg.shape, h.shape[1]
    bm = 256

    def body(dg_ref, du_ref, w_ref, h_ref, y_ref, o_ref):
        part = _nt(dg_ref[:], w_ref[:, 0].reshape(d, ff)) + _nt(du_ref[:], w_ref[:, 1].reshape(d, ff))
        o_ref[:] = _through_norm(h_ref[:], part, y_ref[:])

    return _call(
        body, (s // bm,), [((bm, ff), _row), ((bm, ff), _row), (w.shape, _QUAD), ((bm, d), _row), ((bm, d), _row)], [((bm, d), _row)],
        [_shape((s, d))], 2 * s * d * ff, (dg, du, w, h, by_h),
    )


def back_out(by_h, w):
    s, d = by_h.shape
    n, _, rows, _ = w.shape
    width = n * rows
    bm = 512

    def body(y_ref, w_ref, o_ref):
        o_ref[:] = _nt(y_ref[:], w_ref[:].reshape(width, d)).astype(BF16)

    return _call(
        body, (s // bm,), [((bm, d), _row), ((n, 1, rows, d), _fixed(4, w.shape[1] - 1, 0, 0))], [((bm, width), _row)], [_shape((s, width))], s * d * width, (by_h, w),
    )


def attend_back(qkv, out, lse, by_out, cos, sin):
    _, s, width = qkv.shape
    groups, hb, _ = lse.shape
    b = 512
    half = b // 2
    scale = HEAD**-0.5
    e = scale * LOG2E

    def body(q_ref, k_ref, v_ref, o_ref, y_ref, lse_ref, c_ref, s_ref, d_ref, dq_s, dk_s, dv_s, t_s):
        iq = pl.program_id(1)
        cols = [slice(i * HEAD, (i + 1) * HEAD) for i in range(hb)]
        base = pl.multiple_of(iq * b, b)

        def block(j, nk, rows, diagonal):
            here = pl.ds(j, nk)
            scores = [_nt(k_ref[0, here, c], q_ref[0, rows, c]) for c in cols]
            dps = [_nt(v_ref[0, here, c], y_ref[rows, c]) for c in cols]
            if diagonal:
                shape = (nk, len(range(b)[rows]))
                seen = lax.broadcasted_iota(jnp.int32, shape, 1) >= lax.broadcasted_iota(jnp.int32, shape, 0)
            for i, c in enumerate(cols):
                p = jnp.exp2(scores[i] * e - lse_ref[0, i : i + 1, rows])
                if diagonal:
                    p = jnp.where(seen, p, 0.0)
                ds = (p * (dps[i] - t_s[i : i + 1, rows])).astype(BF16)
                dv = _nn(p.astype(BF16), y_ref[rows, c])
                dk = _nn(ds, q_ref[0, rows, c])
                dv_s[i, here, :] = dv if diagonal else dv_s[i, here, :] + dv
                dk_s[i, here, :] = dk if diagonal else dk_s[i, here, :] + dk
                dq_s[i, :, rows] += _nn(k_ref[0, here, c].T, ds)

        for i, c in enumerate(cols):
            t_s[i : i + 1, :] = (y_ref[:, c].astype(F32) * o_ref[:, c].astype(F32)).T.sum(axis=0, keepdims=True)
        dq_s[:] = jnp.zeros_like(dq_s)
        block(base, half, slice(b), True)
        block(base + half, half, slice(half, b), True)
        _loop(iq, lambda j: block(pl.multiple_of(j * b, b), b, slice(b), False))
        here = pl.ds(base, b)
        for i, c in enumerate(cols):
            d_ref[0, here, c] = _turn_back((dq_s[i] * scale).T, c_ref[here, :], s_ref[here, :])

        @pl.when(iq == pl.num_programs(1) - 1)
        def _():
            def finish(j):
                rows = pl.ds(pl.multiple_of(j * b, b), b)
                for i, c in enumerate(cols):
                    d_ref[1, rows, c] = _turn_back(dk_s[i, rows, :] * scale, c_ref[rows, :], s_ref[rows, :])
                    d_ref[2, rows, c] = dv_s[i, rows, :].astype(BF16)

            _loop(s // b, finish)

    return _call(
        body, (groups, s // b),
        [*_heads(b, s, hb), _few(b, hb), _few(b, hb), _stats(b, hb), ((s, HEAD), _FLAT), ((s, HEAD), _FLAT)],
        [((3, s, hb * HEAD), lambda g, i: (0, 0, g))], [_shape((3, s, width))], 3 * s * s * width, (qkv, qkv, qkv, out, by_out, lse, cos, sin),
        [pltpu.VMEM((hb, HEAD, b), F32), pltpu.VMEM((hb, s, HEAD), F32), pltpu.VMEM((hb, s, HEAD), F32), pltpu.VMEM((hb, b), F32)],
    )


def back_project(d, w, h, by_h):
    (_, s, width), n, rows = d.shape, w.shape[0], w.shape[2]
    dim = h.shape[1]
    bm = 256

    def body(d_ref, w_ref, h_ref, y_ref, o_ref):
        part = sum(_nt(d_ref[m], w_ref[:, m].reshape(dim, width)) for m in range(3))
        o_ref[:] = _through_norm(h_ref[:], part, y_ref[:])

    return _call(
        body, (s // bm,), [((3, bm, width), lambda i: (0, i, 0)), ((n, 3, rows, width), _QUAD), ((bm, dim), _row), ((bm, dim), _row)],
        [((bm, dim), _row)], [_shape((s, dim))], 3 * s * dim * width, (d, w, h, by_h),
    )


def grad_project(a, d, out, by_mid, n):
    (s, dim), width = a.shape, d.shape[2]
    rows, bn = dim // n, 256
    padded = -(-4 * rows // 24) * 24

    def body(a_ref, d_ref, out_ref, m_ref, o_ref):
        which = _step()

        @pl.when(which < 3)
        def _():
            o_ref[:] = _tn(a_ref[:], d_ref[0]).astype(BF16).reshape(n, rows, bn)

        @pl.when(which == 3)
        def _():
            o_ref[:] = _tn(out_ref[:], m_ref[:]).astype(BF16).reshape(n, rows, bn)

    last = width // bn - 1
    return _call(
        body, (4, width // bn),
        [((s, dim), _FLAT), ((1, s, bn), lambda m, i: (jnp.minimum(m, 2), 0, jnp.where(m < 3, i, last))),
         ((s, width), _FLAT), ((s, bn), lambda m, i: (0, jnp.where(m < 3, 0, i)))],
        [((n, rows, bn), lambda m, i: (0, m, i))], [_shape((n, padded, width))], 4 * s * dim * width, (a, d, out, by_mid),
    )


def grad_out(out, by_mid, n):
    (s, width), d = out.shape, by_mid.shape[1]
    rows, bn = width // n, 256

    def body(out_ref, m_ref, o_ref):
        o_ref[:] = _tn(out_ref[:], m_ref[:]).astype(BF16).reshape(n, rows, bn)

    return _call(
        body, (d // bn,), [((s, width), _FLAT), ((s, bn), _col)], [((n, rows, bn), lambda i: (0, 0, i))], [_shape((n, rows, d))],
        s * d * width, (out, by_mid),
    )


def mlp_back(y, w, g, u, act, b, n):
    (s, d), ff = y.shape, w.shape[0]
    rows, bn, third, sub = d // n, 384, ff // 3, 512
    per = third // bn

    def body(y_ref, w_ref, g_ref, u_ref, act_ref, b_ref, dg_ref, du_ref, dn_ref, gu_ref):
        for here in _cuts(s, sub):
            t = _nt(y_ref[here, :], w_ref[:]).astype(BF16).astype(F32)
            gate, up = g_ref[here, :], u_ref[here, :]
            sig = jax.nn.sigmoid(gate)
            part = sig * t
            du_ref[here, :] = (part * gate).astype(BF16)
            dg_ref[here, :] = (part * up * (1 + gate * (1 - sig))).astype(BF16)
        dn_ref[:] = _tn(act_ref[:], y_ref[:]).astype(BF16)
        both = jnp.concatenate([dg_ref[:], du_ref[:]], axis=1)
        for x in range(0, n, 8):
            t = _tn(b_ref[:, x * rows : (x + 8) * rows], both).astype(BF16)
            gu_ref[x : x + 8, 0, 0] = t[:, :bn].reshape(8, rows, bn)
            gu_ref[x : x + 8, 0, 1] = t[:, bn:].reshape(8, rows, bn)

    return _call(
        body, (ff // bn,), [((s, d), _FLAT), ((bn, d), _row), ((s, bn), _col), ((s, bn), _col), ((s, bn), _col), ((s, d), _FLAT)],
        [((s, bn), _col), ((s, bn), _col), ((bn, d), _row), ((n, 1, 2, rows, bn), lambda i: (0, i // per, 0, 0, i % per))],
        [_shape((s, ff)), _shape((s, ff)), _shape((ff, d)), _shape((n, 3, 2, rows, third))], 4 * s * d * ff, (y, w, g, u, act, b),
    )


def after(*values):
    return lax.optimization_barrier(values)


def _tables(tokens):
    half = HEAD // 2
    place = np.arange(max(tokens, half), dtype=np.float32)
    angle = place[:tokens, None] * np.float32(THETA) ** (-place[:half] / np.float32(half))
    c, s = (f(angle.astype(np.float64)).astype(np.float32) for f in (np.cos, np.sin))
    return jnp.asarray(np.concatenate([c, c], -1)), jnp.asarray(np.concatenate([-s, s], -1))


def back_project_and_sum(a, d, g_out, w, h, by_h):
    (_, s, width), dim = d.shape, h.shape[1]
    n, _, rows, _ = w.shape
    bn, bm = 256, 256
    tiles = width // bn
    makes, backs = 3 * tiles, s // bm
    waves = 4

    def body(d_col, a_ref, d_row, h_ref, y_ref, w_hbm, go_hbm, o_ref, sum_ref, w_s, g_s, r0_s, *rest):
        a_s, s1, r1, s2, r2, s3, r3 = (rest[3 * i : 3 * i + 3] for i in range(7))
        w_sem, go_sem, send, recv, core_send, core_recv = rest[21:]
        t = _step()
        bits, core, other, across = _here()

        def at(dims, first, second, third):
            place = [None] * 3
            for dim_, number in zip(dims, (first, second, third)):
                place[dim_] = number
            return tuple(place)

        slot = (1, 0, 1, 0)

        def to_core(wave):
            source = g_s.at[slot[wave], :, :, :, 1 - core] if wave else go_hbm.at[:, :, :, 1 - core]
            return _send(source, r0_s.at[wave], core_send.at[wave], core_recv.at[wave], other)

        def hop(wave, k, stage):
            source, target = ((s1, r1), (s2, r2), (s3, r3))[stage]
            return _send(source[k].at[wave], target[k].at[wave], send.at[wave, stage, k], recv.at[wave, stage, k], across[_order(wave, k)[stage]])

        def mine_of_out():
            return pltpu.make_async_copy(go_hbm.at[:, :, :, core], g_s.at[1, :, :, :, core], go_sem)

        def weights():
            return pltpu.make_async_copy(w_hbm.at[:, pl.ds(0, 3)], w_s, w_sem)

        def add0(wave):
            to_core(wave).wait()
            if wave == 0:
                mine_of_out().wait()
            for k, part in enumerate(PARTS):
                dims = _order(wave, k)
                b = bits[dims[0]]

                def pair(i):
                    second, third = i // 2, i % 2

                    def total(first):
                        p = at(dims, first, second, third)
                        return g_s[(slot[wave], *p, core, ALL, part)].astype(F32) + r0_s[(wave, *p, ALL, part)].astype(F32)

                    s1[k][wave, second, third] = total(1 - b).astype(BF16)
                    a_s[k][wave, second, third] = total(b)

                _loop(4, pair)
            for k in WAYS:
                hop(wave, k, 0).start()

        def add1(wave):
            for k in WAYS:
                hop(wave, k, 0).wait_recv()
                b = bits[_order(wave, k)[1]]

                def one(third):
                    s2[k][wave, third] = (a_s[k][wave, 1 - b, third] + r1[k][wave, 1 - b, third].astype(F32)).astype(BF16)
                    a_s[k][wave, b, third] = a_s[k][wave, b, third] + r1[k][wave, b, third].astype(F32)

                _loop(2, one)
            for k in WAYS:
                hop(wave, k, 1).start()

        def add2(wave):
            for k in WAYS:
                hop(wave, k, 1).wait_recv()
                dims = _order(wave, k)
                b, c = bits[dims[1]], bits[dims[2]]
                s3[k][wave] = (a_s[k][wave, b, 1 - c] + r2[k][wave, 1 - c].astype(F32)).astype(BF16)
                a_s[k][wave, b, c] = a_s[k][wave, b, c] + r2[k][wave, c].astype(F32)
            for k in WAYS:
                hop(wave, k, 2).start()

        def add3(wave):
            for k, part in enumerate(PARTS):
                hop(wave, k, 2).wait_recv()
                dims = _order(wave, k)
                b, c = bits[dims[1]], bits[dims[2]]
                sum_ref[wave, :, part] = (a_s[k][wave, b, c] + r3[k][wave].astype(F32)).astype(BF16)

        @pl.when(t == 0)
        def _():
            _meet((other, *across))
            to_core(0).start()
            mine_of_out().start()
            weights().start()

        @pl.when(t < makes)
        def _():
            made = _tn(a_ref[:], d_col[0]).astype(BF16).reshape(*TORUS, rows, bn)
            for i in range(tiles):

                @pl.when(t % tiles == i)
                def _():
                    g_s[(t // tiles) % 2, :, :, :, :, :, i * bn : (i + 1) * bn] = made

        @pl.when(t == makes)
        def _():
            weights().wait()

        @pl.when(t >= makes)
        def _():
            part = sum(_nt(d_row[m], w_s[:, m].reshape(dim, width)) for m in range(3))
            o_ref[:] = _through_norm(h_ref[:], part, y_ref[:])

        last = makes + backs - 1
        for wave in range(waves):
            steps = ((add0, 4 * wave + 3), (add1, 3 * wave + 9), (add2, min(3 * wave + 14, last - 1)), (add3, min(3 * wave + 17, last)))
            for action, step in steps + (((lambda i: to_core(i).start()), tiles * wave - 1),) * (wave > 0):
                pl.when(t == step)(functools.partial(action, wave))

        @pl.when(t == last)
        def _():
            for wave in range(waves):
                for stage in WAYS:
                    for k in WAYS:
                        hop(wave, k, stage).wait_send()

    def made(t):
        return jnp.minimum(t, makes - 1)

    def back(t):
        return jnp.maximum(t - makes, 0)

    wide = [part.stop - part.start for part in PARTS]
    tile = lambda t: (back(t), 0)
    total, summed = pl.pallas_call(
        body,
        grid=(makes + backs,),
        in_specs=[
            pl.BlockSpec((1, s, bn), lambda t: (made(t) // tiles, 0, made(t) % tiles)), _spec((s, dim), _FLAT),
            pl.BlockSpec((3, bm, width), lambda t: (0, back(t), 0)), pl.BlockSpec((bm, dim), tile), pl.BlockSpec((bm, dim), tile),
            ANY, ANY,
        ],
        out_specs=[pl.BlockSpec((bm, dim), tile), pl.BlockSpec((waves, rows, width), _CUBE)],
        out_shape=[_shape((s, dim)), _shape((waves, rows, width))],
        scratch_shapes=[
            pltpu.VMEM((n, 3, rows, width), BF16), pltpu.VMEM((2, *TORUS, rows, width), BF16), pltpu.VMEM((waves, *TORUS[1:], rows, width), BF16),
            *(pltpu.VMEM((waves, 2, 2, rows, x), F32) for x in wide),
            *(pltpu.VMEM((waves, *((2,) * (2 - i)), rows, x), BF16) for i in WAYS for _ in range(2) for x in wide),
            pltpu.SemaphoreType.DMA, pltpu.SemaphoreType.DMA, *_link_sems(waves),
        ],
        compiler_params=pltpu.CompilerParams(vmem_limit_bytes=VMEM, dimension_semantics=("arbitrary",), collective_id=0, has_side_effects=True),
        cost_estimate=pl.CostEstimate(flops=12 * s * dim * width, bytes_accessed=60 * 2**20, transcendentals=0),
    )(d, a, d, h, by_h, w, g_out.reshape(*TORUS, rows, width))
    return total, summed


def solution(mesh):
    n = mesh.shape["dp"]

    def gather(t):
        return lax.all_gather(t, "dp", axis=0, tiled=True)

    def scatter(t):
        flat = lax.psum_scatter(t.reshape(-1, t.shape[-1]), "dp", scatter_dimension=0, tiled=True)
        return flat.reshape(t.shape[1:])

    def step(x, dy, wq, wk, wv, wo, w_gate, w_up, w_down):
        layers, rows, width = wq.shape
        ff = w_gate.shape[2]
        s = x.shape[1]
        cos, sin = _tables(s)
        h = x[0]
        kept = []
        for l in range(layers):
            w_out = None if l else gather(wo[l]).reshape(n, 1, rows, width)
            w_gu = gather(jnp.concatenate([w_gate[l], w_up[l]], axis=0)).reshape(n, 2, rows, ff)
            if l:
                w_qkvo = gather(jnp.concatenate([wq[l], wk[l], wv[l], wo[l]], axis=0)).reshape(n, 4, rows, width)
                w_dn = gather(w_down[l])
                qkv, w_out = project(a, w_qkvo, cos, sin), w_qkvo
            else:
                a, qkv, w_qkvo = fetch_and_project(h, cos, sin, wq, wk, wv)
            out, lse = attend(qkv)
            mid, b = add_matmul(out, w_out, h, (n, 1, rows, width), (0, w_out.shape[1] - 1, 0, 0))
            if l:
                g, u, act = gate_up(b, w_gu)
            else:
                g, u, act, w_dn = gate_up(b, w_gu, w_down[l])
            kept.append((w_qkvo, w_out, w_gu, w_dn, h, a, qkv, out, lse, mid, b, g, u, act))
            if l + 1 < layers:
                h, a = add_matmul(act, w_dn, mid)

        y = dy[0]
        grads = []
        for l in reversed(range(layers)):
            w_qkvo, w_out, w_gu, w_dn, h, a, qkv, out, lse, mid, b, g, u, act = kept[l]
            dg, du, g_dn, g_gu = mlp_back(y, w_dn, g, u, act, b, n)
            of_gu = scatter(g_gu)
            of_dn = scatter(g_dn.reshape(n, -1, g_dn.shape[1]))
            y_mid = back_gate_up(dg, du, w_gu, mid, y)
            if l == 0:
                g_out, y_mid = after(grad_out(out, y_mid, n), y_mid)
            d = attend_back(qkv, out, lse, back_out(y_mid, w_out), cos, sin)
            if l == 0:
                y, sums = back_project_and_sum(a, d, g_out, w_qkvo, h, y_mid)
                grads.append((sums[1], sums[2], sums[3], sums[0], *(jnp.concatenate(list(of_gu[:, i]), axis=-1) for i in (0, 1)), of_dn))
                break
            g_qkvo, d = after(grad_project(a, d, out, y_mid, n), d)
            of_qkvo = scatter(g_qkvo)
            y = back_project(d, w_qkvo, h, y_mid)
            grads.append((*(of_qkvo[i * rows : (i + 1) * rows] for i in range(4)), *(jnp.concatenate(list(of_gu[:, i]), axis=-1) for i in (0, 1)), of_dn))
        grads.reverse()
        return (y[None], *(jnp.stack([g[i] for g in grads]) for i in range(7)))

    states, cut = P(("rep", "dp"), None, None), P(None, "dp", None)
    return jax.shard_map(
        step,
        mesh=mesh,
        in_specs=(states, states) + (cut,) * 7,
        out_specs=(states,) + (P("rep", "dp", None),) * 7,
        check_vma=False,
    )
```

```python
import functools

import jax
import jax.numpy as jnp
import numpy as np
from jax import lax
from jax.experimental import pallas as pl
from jax.experimental.pallas import tpu as pltpu
from jax.sharding import PartitionSpec as P


HEAD = 128
THETA = 10000
EPS = 1e-6
LOG2E = 1.4426950408889634
HIDDEN = -2e30
LOW = -1e30
VMEM = 60 * 2**20
BF16, F32 = jnp.bfloat16, jnp.float32


def _dot(a, b, ca, cb):
    return lax.dot_general(a, b, (((ca,), (cb,)), ((), ())), preferred_element_type=F32)


def _nn(a, b):
    return _dot(a, b, 1, 0)


def _nt(a, b):
    return _dot(a, b, 1, 1)


def _tn(a, b):
    return _dot(a, b, 0, 0)


def _row(i):
    return i, 0


def _col(i):
    return 0, i


class _fixed:
    def __init__(self, rank, *last):
        self.place = (0,) * (rank - len(last)) + last

    def __call__(self, *_):
        return self.place


def _spec(block, index):
    if block is None:
        return ANY
    return pl.BlockSpec(block, index, pipeline_mode=pl.Buffered(1)) if isinstance(index, _fixed) else pl.BlockSpec(block, index)


def _step():
    return pl.program_id(0)


def _cuts(size, step):
    return [slice(x, min(x + step, size)) for x in range(0, size, step)]


def _loop(count, body):
    lax.fori_loop(0, count, lambda i, _: body(i), None)


_FLAT, _CUBE, _QUAD = _fixed(2), _fixed(3), _fixed(4)


def _call(body, grid, ins, outs, shapes, work, args, scratch=(), carry=None):
    moved = sum(a.size * a.dtype.itemsize for a in (*args, *shapes))
    params = {"vmem_limit_bytes": VMEM, "dimension_semantics": ("arbitrary",) * len(grid)}
    ins, outs, shapes, args, scratch = [_spec(*x) for x in ins], [_spec(*x) for x in outs], list(shapes), list(args), list(scratch)
    if carry:
        body = carry.beside(body, len(ins), len(outs))
        ins, args, outs, shapes, scratch = [*ins, ANY], [*args, carry.shard], [*outs, ANY], [*shapes, carry.shape()], [*carry.scratch(), *scratch]
        params |= {"collective_id": carry.number, "has_side_effects": True}
    results = pl.pallas_call(
        body,
        grid=grid,
        in_specs=ins,
        out_specs=outs,
        out_shape=shapes,
        scratch_shapes=scratch,
        compiler_params=pltpu.CompilerParams(**params),
        cost_estimate=pl.CostEstimate(flops=2 * work, bytes_accessed=moved, transcendentals=0),
    )(*args)
    return results if len(shapes) > 1 else results[0]


def _shape(shape, dtype=BF16):
    return jax.ShapeDtypeStruct(shape, dtype)


def _scale(wide):
    return lax.rsqrt(jnp.mean(wide * wide, -1, keepdims=True) + EPS)


def _sum_and_normed(h, part):
    total = (h.astype(F32) + part.astype(BF16).astype(F32)).astype(BF16)
    wide = total.astype(F32)
    return total, (wide * _scale(wide)).astype(BF16)


def _through_norm(h, by_b, by_h):
    wide, c = h.astype(F32), by_b.astype(BF16).astype(F32)
    r = _scale(wide)
    along = jnp.sum(c * wide, -1, keepdims=True)
    part = (c * r - wide * (along * (r * r * r) / wide.shape[-1])).astype(BF16)
    return (by_h.astype(F32) + part.astype(F32)).astype(BF16)


def _turn(t, cos, sin):
    x = t.astype(F32)
    return (x * cos + pltpu.roll(x, HEAD // 2, 1) * sin).astype(BF16)


def _turn_back(t, cos, sin):
    x = t.astype(BF16).astype(F32)
    return (x * cos - pltpu.roll(x, HEAD // 2, 1) * sin).astype(BF16)


PARTS = (slice(0, 384), slice(384, 768), slice(768, 1280))
ANY = pl.BlockSpec(memory_space=pl.ANY)
TORUS = (2, 2, 2, 2)
WAYS = range(3)
ALL = slice(None)


def _here():
    me = lax.axis_index("dp")
    bits = [me // 8, me // 4 % 2, me // 2 % 2]
    core = me % 2
    return bits, core, me + 1 - 2 * core, [me + far * (1 - 2 * b) for far, b in zip((8, 4, 2), bits)]


def _order(wave, k):
    return [(k + wave + i) % 3 for i in WAYS]


def _send(source, target, sent, came, device):
    return pltpu.make_async_remote_copy(
        src_ref=source, dst_ref=target, send_sem=sent, recv_sem=came, device_id={"dp": device}, device_id_type=pl.DeviceIdType.MESH
    )


def _meet(devices):
    barrier = pltpu.get_barrier_semaphore()
    for device in devices:
        pl.semaphore_signal(barrier, inc=1, device_id={"dp": device}, device_id_type=pl.DeviceIdType.MESH)
    pl.semaphore_wait(barrier, len(devices))


def _link_sems(waves):
    return [pltpu.SemaphoreType.DMA((waves, 3, 3))] * 2 + [pltpu.SemaphoreType.DMA((waves,))] * 2


class _Spread:
    def __init__(self, own, whole, pick, sems):
        self.own, self.whole, self.pick = own, whole, pick
        self.sent, self.came, self.core_sent, self.core_came, self.stored = sems
        self.bits, self.core, self.other, self.across = _here()

    def _hop(self, wave, stage, k):
        dims = _order(wave, k)
        place = [ALL if i in dims[:stage] else b for i, b in enumerate(self.bits)]
        target = self.whole.at[(*place, self.core, *self.pick[wave], PARTS[k])]
        source = target if stage else self.own.at[(*self.pick[wave], PARTS[k])]
        return _send(source, target, self.sent.at[wave, stage, k], self.came.at[wave, stage, k], self.across[dims[stage]])

    def _to_core(self, wave):
        mine = self.whole.at[(*[ALL] * 3, self.core, *self.pick[wave])]
        return _send(mine, mine, self.core_sent.at[wave], self.core_came.at[wave], self.other)

    def _store(self, wave):
        return pltpu.make_async_copy(self.own.at[self.pick[wave]], self.whole.at[(*self.bits, self.core, *self.pick[wave])], self.stored.at[wave])

    def start(self, wave, stage=0):
        for k in WAYS:
            if stage:
                self._hop(wave, stage - 1, k).wait_recv()
        if stage == 1:
            self._store(wave).wait()
        for k in WAYS:
            if stage < 3:
                self._hop(wave, stage, k).start()
        if stage == 0:
            self._store(wave).start()
        if stage == 3:
            self._to_core(wave).start()

    def finish(self, wave):
        self._to_core(wave).wait()
        for stage in WAYS:
            for k in WAYS:
                self._hop(wave, stage, k).wait_send()


class _Carry:
    def __init__(self, shard, number, depth=56):
        self.shard, self.number, self.block = shard, number, shard.shape[1:]
        self.pick = [(rows,) for rows in _cuts(self.block[0], depth)]

    def shape(self):
        return _shape((*TORUS, *self.block))

    def scratch(self):
        waves = len(self.pick)
        return [pltpu.VMEM(self.block, BF16), pltpu.SemaphoreType.DMA, *_link_sems(waves), pltpu.SemaphoreType.DMA((waves,))]

    def beside(self, body, n_in, n_out):
        count = len(self.scratch())

        def both(*refs):
            t = _step()
            shard, outs, (whole, own_s, own_sem, *rest) = refs[n_in], refs[n_in + 1 :][:n_out], refs[n_in + 1 + n_out :]
            sems, scratch = rest[: count - 2], rest[count - 2 :]
            spread = _Spread(own_s, whole, self.pick, sems)

            @pl.when(t == 0)
            def _():
                own = pltpu.make_async_copy(shard.at[0], own_s, own_sem)
                own.start()
                _meet((spread.other, *spread.across))
                own.wait()
                for wave in range(len(self.pick)):
                    spread.start(wave)

            body(*refs[:n_in], *outs, *scratch)
            for stage in WAYS:
                for wave in range(len(self.pick)):
                    pl.when(t == wave + 2 * stage)(functools.partial(spread.start, wave, stage + 1))

            @pl.when(t == pl.num_programs(0) - 1)
            def _():
                for wave in range(len(self.pick)):
                    spread.finish(wave)

        return both


def fetch_and_project(x, cos, sin, shards, packs):
    (s, d), (_, rows, width) = x.shape, shards[0].shape
    n, waves, bm, sub = 16, len(shards), s // 2, 256
    loose = [x for pack in packs for x in pack]
    packed = [_shape((len(pack) * pack[0].shape[1], pack[0].shape[2])) for pack in packs]

    def body(x_hbm, c_ref, s_ref, *rest):
        parts, rest = rest[:waves], rest[waves:]
        loose_, rest = rest[: len(loose)], rest[len(loose) :]
        (a_ref, o_ref, whole), packed_, rest = rest[:3], rest[3 : 3 + len(packs)], rest[3 + len(packs) :]
        held, (own_s, x_s, w_s, own_sem, x_sem, w_sem, came, left), sems = rest[: len(packs)], rest[len(packs) : -5], rest[-5:]
        t = _step()
        spread = _Spread(own_s, whole, [(i, ALL) for i in range(waves)], sems)

        def own(i):
            return pltpu.make_async_copy(parts[i].at[0], own_s.at[i], own_sem.at[i])

        def states():
            return pltpu.make_async_copy(x_hbm, x_s, x_sem)

        def weights(i):
            return pltpu.make_async_copy(whole.at[(*[ALL] * len(TORUS), i)], w_s.at[i % 2], w_sem)

        def bring():
            of = [(k, i) for k, pack in enumerate(packs) for i in range(len(pack))]
            rows_ = [pack[0].shape[1] for pack in packs]
            return [
                pltpu.make_async_copy(loose_[j].at[1], held[k].at[pl.ds(i * rows_[k], rows_[k])], came.at[j]) for j, (k, i) in enumerate(of)
            ]

        def put():
            return [pltpu.make_async_copy(held[k], packed_[k], left.at[k]) for k in range(len(packs))]

        def ready(i):
            spread.finish(i)
            weights(i).start()
            weights(i).wait()

        def begin():
            for i in range(waves):
                own(i).start()
            states().start()
            _meet((spread.other, *spread.across))
            for i in range(waves):
                own(i).wait()
                spread.start(i)
            states().wait()

            def norm(i):
                here = pl.ds(pl.multiple_of(i * sub, sub), sub)
                wide = x_s[here, :].astype(F32)
                a_ref[here, :] = (wide * _scale(wide)).astype(BF16)

            for copy in bring():
                copy.start()
            _loop(s // sub, norm)
            spread.start(0, 1)
            spread.start(1, 1)
            for copy in bring():
                copy.wait()
            for copy in put():
                copy.start()
            spread.start(0, 2)
            spread.start(2, 1)
            spread.start(1, 2)
            spread.start(0, 3)
            for copy in put():
                copy.wait()
            ready(0)

        pl.when(t == 0)(begin)

        def run(turn, matrix, half):
            ww = w_s[matrix % 2].reshape(d, width)
            for r in range(0, bm, sub):
                here = pl.ds(pl.multiple_of(half * bm + r, sub), sub)
                y = _nn(a_ref[here, :], ww).astype(BF16)
                if turn:
                    c, sn = c_ref[here, :], s_ref[here, :]
                    for k in range(0, width, HEAD):
                        o_ref[0, r : r + sub, k : k + HEAD] = _turn(y[:, k : k + HEAD], c, sn)
                else:
                    o_ref[0, r : r + sub, :] = y

        matrix, half = (t - 1) // 2, (t + 1) % 2
        pl.when((t > 0) & (matrix < 2))(lambda: run(True, matrix, half))
        pl.when(matrix == 2)(lambda: run(False, matrix, half))
        after_step = (), ((spread.start, 2, 2), (spread.start, 1, 3)), ((ready, 1),), ((spread.start, 2, 3),), ((ready, 2),)
        for step, actions in enumerate(after_step):

            @pl.when(t == step)
            def _():
                for action, *args in actions:
                    action(*args)

    def at(t):
        return jnp.maximum(t - 1, 0)

    a, qkv, whole, *packed = pl.pallas_call(
        body,
        grid=(7,),
        in_specs=[ANY, *[_spec((s, HEAD), _FLAT)] * 2, *[ANY] * (waves + len(loose))],
        out_specs=[pl.BlockSpec((s, d), _FLAT), pl.BlockSpec((1, bm, width), lambda t: (at(t) // 2, at(t) % 2, 0)), *[ANY] * (1 + len(packs))],
        out_shape=[_shape((s, d)), _shape((3, s, width)), _shape((*TORUS, waves, rows, width)), *packed],
        scratch_shapes=[
            *(pltpu.VMEM(x.shape, BF16) for x in packed),
            pltpu.VMEM((waves, rows, width), BF16), pltpu.VMEM((s, d), BF16), pltpu.VMEM((2, *TORUS, rows, width), BF16),
            pltpu.SemaphoreType.DMA((waves,)), pltpu.SemaphoreType.DMA, pltpu.SemaphoreType.DMA,
            pltpu.SemaphoreType.DMA((len(loose),)), pltpu.SemaphoreType.DMA((len(packs),)), *_link_sems(waves), pltpu.SemaphoreType.DMA((waves,)),
        ],
        compiler_params=pltpu.CompilerParams(vmem_limit_bytes=VMEM, collective_id=1, has_side_effects=True),
        cost_estimate=pl.CostEstimate(flops=12 * s * d * width, bytes_accessed=VMEM, transcendentals=0),
    )(x, cos, sin, *shards, *loose)
    return a, qkv, whole.reshape(n, waves, rows, width), packed


def project(a, w, cos, sin):
    (s, d), (n, _, rows, width) = a.shape, w.shape
    bm, sub = min(1024, s), 256

    def body(a_ref, w_ref, c_ref, s_ref, o_ref):
        which, at = _step(), pl.program_id(1)
        ww = w_ref[:].reshape(d, width)

        def run(turn):
            for r in range(0, bm, sub):
                t = _nn(a_ref[r : r + sub, :], ww).astype(BF16)
                if turn:
                    here = pl.ds(at * bm + r, sub)
                    c, sn = c_ref[here, :], s_ref[here, :]
                    for x in range(0, width, HEAD):
                        o_ref[0, r : r + sub, x : x + HEAD] = _turn(t[:, x : x + HEAD], c, sn)
                else:
                    o_ref[0, r : r + sub, :] = t

        pl.when(which < 2)(lambda: run(True))
        pl.when(which == 2)(lambda: run(False))

    return _call(
        body, (3, s // bm),
        [((bm, d), lambda m, i: (i, 0)), ((n, 1, rows, width), lambda m, i: (0, m, 0, 0)), ((s, HEAD), _FLAT), ((s, HEAD), _FLAT)],
        [((1, bm, width), lambda m, i: (m, i, 0))], [_shape((3, s, width))], 3 * s * d * width, (a, w, cos, sin),
    )


def _seen(keys, queries):
    place = [lax.broadcasted_iota(jnp.int32, (keys, queries), i) for i in (0, 1)]
    return place[1] >= place[0]


def _heads(b, s, hb):
    return [((1, b, hb * HEAD), lambda g, i: (0, i, g)), *(((1, s, hb * HEAD), lambda g, i, m=m: (m, 0, g)) for m in (1, 2))]


def _few(b, hb):
    return (b, hb * HEAD), lambda g, i: (i, g)


def _stats(b, hb):
    return (1, hb, b), lambda g, i: (g, 0, i)


def attend(qkv):
    _, s, width = qkv.shape
    heads = width // HEAD
    hb, b = 5, 512
    half = b // 2
    e = HEAD**-0.5 * LOG2E

    def body(q_ref, k_ref, v_ref, o_ref, lse_ref, top_s, mix_s):
        iq = pl.program_id(1)
        cols = [slice(i * HEAD, (i + 1) * HEAD) for i in range(hb)]
        top_s[:] = jnp.full(top_s.shape, LOW, F32)
        mix_s[:] = jnp.zeros(mix_s.shape, F32)

        def block(j, nk, rows, diagonal):
            here = pl.ds(j, nk)
            ones = jnp.ones((8, nk), BF16)
            scores = [_nt(k_ref[0, here, c], q_ref[0, rows, c]) for c in cols]
            if diagonal:
                seen = _seen(nk, len(range(b)[rows]))
            weights, keeps = [], []
            for i, x in enumerate(scores):
                if diagonal:
                    x = jnp.where(seen, x, HIDDEN)
                old = top_s[i : i + 1, rows]
                top = jnp.maximum(old, x.max(axis=0, keepdims=True))
                top_s[i : i + 1, rows] = top
                weights.append(jnp.exp2((x - top) * e).astype(BF16))
                keeps.append(jnp.exp2((old - top) * e))
            for i, (c, p, keep) in enumerate(zip(cols, weights, keeps)):
                values = jnp.concatenate([v_ref[0, here, c].T, ones], axis=0)
                mix_s[i, :, rows] = mix_s[i, :, rows] * keep + _nn(values, p)

        base = pl.multiple_of(iq * b, b)
        _loop(iq, lambda j: block(pl.multiple_of(j * b, b), b, slice(b), False))
        block(base, half, slice(b), True)
        block(base + half, half, slice(half, b), True)
        for i, c in enumerate(cols):
            total = mix_s[i, HEAD : HEAD + 1, :]
            o_ref[:, c] = (mix_s[i, :HEAD, :] * (1 / total)).T.astype(BF16)
            lse_ref[0, i : i + 1, :] = top_s[i : i + 1, :] * e + jnp.log2(total)

    return _call(
        body, (heads // hb, s // b), _heads(b, s, hb), [_few(b, hb), _stats(b, hb)],
        [_shape((s, width)), _shape((heads // hb, hb, s), F32)], s * s * width, (qkv, qkv, qkv),
        [pltpu.VMEM((hb, b), F32), pltpu.VMEM((hb, HEAD + 8, b), F32)],
    )


def add_matmul(a, w, h, block=None, at=None):
    s, d, width = a.shape[0], a.shape[1], h.shape[1]
    bm, sub = 512, 256
    block, at = block or w.shape, at or (0,) * w.ndim

    def body(a_ref, w_ref, h_ref, o_ref, b_ref):
        ww = w_ref[:].reshape(d, width)
        for here in _cuts(bm, sub):
            o_ref[here, :], b_ref[here, :] = _sum_and_normed(h_ref[here, :], _nn(a_ref[here, :], ww))

    return _call(
        body, (s // bm,), [((bm, d), _row), (block, _fixed(len(at), *at)), ((bm, width), _row)], [((bm, width), _row)] * 2,
        [_shape((s, width))] * 2, s * d * width, (a, w, h),
    )


def gate_up(b, w, carry=None):
    (s, d), (n, _, rows, ff) = b.shape, w.shape
    bn, sub = 384, 256

    def body(b_ref, w_ref, g_ref, u_ref, act_ref):
        ww = jnp.concatenate([w_ref[:, 0].reshape(d, bn), w_ref[:, 1].reshape(d, bn)], axis=1)
        for here in _cuts(s, sub):
            t = _nn(b_ref[here, :], ww)
            g, u = t[:, :bn], t[:, bn:]
            g_ref[here, :] = g
            u_ref[here, :] = u
            act_ref[here, :] = (g * jax.nn.sigmoid(g) * u).astype(BF16)

    return _call(
        body, (ff // bn,), [((s, d), _FLAT), ((n, 2, rows, bn), lambda i: (0, 0, 0, i))], [((s, bn), _col)] * 3,
        [_shape((s, ff), F32), _shape((s, ff), F32), _shape((s, ff))], 2 * s * d * ff, (b, w), carry=carry,
    )


def back_gate_up(dg, du, w, h, by_h):
    (s, ff), d = dg.shape, h.shape[1]
    bm = 256

    def body(dg_ref, du_ref, w_ref, h_ref, y_ref, o_ref):
        part = _nt(dg_ref[:], w_ref[:, 0].reshape(d, ff)) + _nt(du_ref[:], w_ref[:, 1].reshape(d, ff))
        o_ref[:] = _through_norm(h_ref[:], part, y_ref[:])

    return _call(
        body, (s // bm,), [((bm, ff), _row), ((bm, ff), _row), (w.shape, _QUAD), ((bm, d), _row), ((bm, d), _row)], [((bm, d), _row)],
        [_shape((s, d))], 2 * s * d * ff, (dg, du, w, h, by_h),
    )


def back_out(by_h, w):
    s, d = by_h.shape
    n, _, rows, _ = w.shape
    width = n * rows
    bm = 512

    def body(y_ref, w_ref, o_ref):
        o_ref[:] = _nt(y_ref[:], w_ref[:].reshape(width, d)).astype(BF16)

    return _call(
        body, (s // bm,), [((bm, d), _row), ((n, 1, rows, d), _fixed(4, w.shape[1] - 1, 0, 0))], [((bm, width), _row)], [_shape((s, width))], s * d * width, (by_h, w),
    )


def attend_back(qkv, out, lse, by_out, cos, sin):
    _, s, width = qkv.shape
    groups, hb, _ = lse.shape
    b = 512
    half = b // 2
    scale = HEAD**-0.5
    e = scale * LOG2E

    def body(q_ref, k_ref, v_ref, o_ref, y_ref, lse_ref, c_ref, s_ref, d_ref, dq_s, dk_s, dv_s, t_s):
        iq = pl.program_id(1)
        cols = [slice(i * HEAD, (i + 1) * HEAD) for i in range(hb)]
        base = pl.multiple_of(iq * b, b)

        def block(j, nk, rows, diagonal):
            here = pl.ds(j, nk)
            scores = [_nt(k_ref[0, here, c], q_ref[0, rows, c]) for c in cols]
            dps = [_nt(v_ref[0, here, c], y_ref[rows, c]) for c in cols]
            if diagonal:
                seen = _seen(nk, len(range(b)[rows]))
            for i, c in enumerate(cols):
                p = jnp.exp2(scores[i] * e - lse_ref[0, i : i + 1, rows])
                if diagonal:
                    p = jnp.where(seen, p, 0.0)
                ds = (p * (dps[i] - t_s[i : i + 1, rows])).astype(BF16)
                dv = _nn(p.astype(BF16), y_ref[rows, c])
                dk = _nn(ds, q_ref[0, rows, c])
                dv_s[i, here, :] = dv if diagonal else dv_s[i, here, :] + dv
                dk_s[i, here, :] = dk if diagonal else dk_s[i, here, :] + dk
                dq_s[i, :, rows] += _nn(k_ref[0, here, c].T, ds)

        for i, c in enumerate(cols):
            t_s[i : i + 1, :] = (y_ref[:, c].astype(F32) * o_ref[:, c].astype(F32)).T.sum(axis=0, keepdims=True)
        dq_s[:] = jnp.zeros_like(dq_s)
        block(base, half, slice(b), True)
        block(base + half, half, slice(half, b), True)
        _loop(iq, lambda j: block(pl.multiple_of(j * b, b), b, slice(b), False))
        here = pl.ds(base, b)
        for i, c in enumerate(cols):
            d_ref[0, here, c] = _turn_back((dq_s[i] * scale).T, c_ref[here, :], s_ref[here, :])

        @pl.when(iq == pl.num_programs(1) - 1)
        def _():
            def finish(j):
                rows = pl.ds(pl.multiple_of(j * b, b), b)
                for i, c in enumerate(cols):
                    d_ref[1, rows, c] = _turn_back(dk_s[i, rows, :] * scale, c_ref[rows, :], s_ref[rows, :])
                    d_ref[2, rows, c] = dv_s[i, rows, :].astype(BF16)

            _loop(s // b, finish)

    return _call(
        body, (groups, s // b),
        [*_heads(b, s, hb), _few(b, hb), _few(b, hb), _stats(b, hb), ((s, HEAD), _FLAT), ((s, HEAD), _FLAT)],
        [((3, s, hb * HEAD), lambda g, i: (0, 0, g))], [_shape((3, s, width))], 3 * s * s * width, (qkv, qkv, qkv, out, by_out, lse, cos, sin),
        [pltpu.VMEM((hb, HEAD, b), F32), pltpu.VMEM((hb, s, HEAD), F32), pltpu.VMEM((hb, s, HEAD), F32), pltpu.VMEM((hb, b), F32)],
    )


def back_project(d, w, h, by_h):
    (_, s, width), n, rows = d.shape, w.shape[0], w.shape[2]
    dim = h.shape[1]
    bm = 256

    def body(d_ref, w_ref, h_ref, y_ref, o_ref):
        part = sum(_nt(d_ref[m], w_ref[:, m].reshape(dim, width)) for m in range(3))
        o_ref[:] = _through_norm(h_ref[:], part, y_ref[:])

    return _call(
        body, (s // bm,), [((3, bm, width), lambda i: (0, i, 0)), ((n, 3, rows, width), _QUAD), ((bm, dim), _row), ((bm, dim), _row)],
        [((bm, dim), _row)], [_shape((s, dim))], 3 * s * dim * width, (d, w, h, by_h),
    )


def grad_project(a, d, out, by_mid, n):
    (s, dim), width = a.shape, d.shape[2]
    rows, bn = dim // n, 256
    padded = -(-4 * rows // 24) * 24

    def body(a_ref, d_ref, out_ref, m_ref, o_ref):
        which = _step()

        @pl.when(which < 3)
        def _():
            o_ref[:] = _tn(a_ref[:], d_ref[0]).astype(BF16).reshape(n, rows, bn)

        @pl.when(which == 3)
        def _():
            o_ref[:] = _tn(out_ref[:], m_ref[:]).astype(BF16).reshape(n, rows, bn)

    last = width // bn - 1
    return _call(
        body, (4, width // bn),
        [((s, dim), _FLAT), ((1, s, bn), lambda m, i: (jnp.minimum(m, 2), 0, jnp.where(m < 3, i, last))),
         ((s, width), _FLAT), ((s, bn), lambda m, i: (0, jnp.where(m < 3, 0, i)))],
        [((n, rows, bn), lambda m, i: (0, m, i))], [_shape((n, padded, width))], 4 * s * dim * width, (a, d, out, by_mid),
    )


def grad_out(out, by_mid, n):
    (s, width), d = out.shape, by_mid.shape[1]
    rows, bn = width // n, 256

    def body(out_ref, m_ref, o_ref):
        o_ref[:] = _tn(out_ref[:], m_ref[:]).astype(BF16).reshape(n, rows, bn)

    return _call(
        body, (d // bn,), [((s, width), _FLAT), ((s, bn), _col)], [((n, rows, bn), lambda i: (0, 0, i))], [_shape((n, rows, d))],
        s * d * width, (out, by_mid),
    )


def mlp_back(y, w, g, u, act, b, n):
    (s, d), ff = y.shape, w.shape[0]
    rows, bn, third, sub = d // n, 384, ff // 3, 512
    per = third // bn

    def body(y_ref, w_ref, g_ref, u_ref, act_ref, b_ref, dg_ref, du_ref, dn_ref, gu_ref):
        for here in _cuts(s, sub):
            t = _nt(y_ref[here, :], w_ref[:]).astype(BF16).astype(F32)
            gate, up = g_ref[here, :], u_ref[here, :]
            sig = jax.nn.sigmoid(gate)
            part = sig * t
            du_ref[here, :] = (part * gate).astype(BF16)
            dg_ref[here, :] = (part * up * (1 + gate * (1 - sig))).astype(BF16)
        dn_ref[:] = _tn(act_ref[:], y_ref[:]).astype(BF16)
        both = jnp.concatenate([dg_ref[:], du_ref[:]], axis=1)
        for x in range(0, n, 8):
            t = _tn(b_ref[:, x * rows : (x + 8) * rows], both).astype(BF16)
            gu_ref[x : x + 8, 0, 0] = t[:, :bn].reshape(8, rows, bn)
            gu_ref[x : x + 8, 0, 1] = t[:, bn:].reshape(8, rows, bn)

    return _call(
        body, (ff // bn,), [((s, d), _FLAT), ((bn, d), _row), ((s, bn), _col), ((s, bn), _col), ((s, bn), _col), ((s, d), _FLAT)],
        [((s, bn), _col), ((s, bn), _col), ((bn, d), _row), ((n, 1, 2, rows, bn), lambda i: (0, i // per, 0, 0, i % per))],
        [_shape((s, ff)), _shape((s, ff)), _shape((ff, d)), _shape((n, 3, 2, rows, third))], 4 * s * d * ff, (y, w, g, u, act, b),
    )


def after(*values):
    return lax.optimization_barrier(values)


def _tables(tokens):
    half = HEAD // 2
    place = np.arange(max(tokens, half), dtype=np.float32)
    angle = place[:tokens, None] * np.float32(THETA) ** (-place[:half] / np.float32(half))
    c, s = (f(angle.astype(np.float64)).astype(np.float32) for f in (np.cos, np.sin))
    return jnp.asarray(np.concatenate([c, c], -1)), jnp.asarray(np.concatenate([-s, s], -1))


def back_project_and_sum(a, d, g_out, w, h, by_h):
    (_, s, width), dim = d.shape, h.shape[1]
    n, _, rows, _ = w.shape
    bn, bm = 256, 256
    tiles = width // bn
    makes, backs = 3 * tiles, s // bm
    waves = 4

    def body(d_col, a_ref, d_row, h_ref, y_ref, w_hbm, go_hbm, o_ref, sum_ref, w_s, g_s, r0_s, *rest):
        a_s, s1, r1, s2, r2, s3, r3 = (rest[3 * i : 3 * i + 3] for i in range(7))
        w_sem, go_sem, send, recv, core_send, core_recv = rest[21:]
        t = _step()
        bits, core, other, across = _here()

        def at(dims, first, second, third):
            place = [None] * 3
            for dim_, number in zip(dims, (first, second, third)):
                place[dim_] = number
            return tuple(place)

        slot = (1, 0, 1, 0)

        def to_core(wave):
            source = g_s.at[slot[wave], :, :, :, 1 - core] if wave else go_hbm.at[:, :, :, 1 - core]
            return _send(source, r0_s.at[wave], core_send.at[wave], core_recv.at[wave], other)

        def hop(wave, k, stage):
            source, target = ((s1, r1), (s2, r2), (s3, r3))[stage]
            return _send(source[k].at[wave], target[k].at[wave], send.at[wave, stage, k], recv.at[wave, stage, k], across[_order(wave, k)[stage]])

        def mine_of_out():
            return pltpu.make_async_copy(go_hbm.at[:, :, :, core], g_s.at[1, :, :, :, core], go_sem)

        def weights():
            return pltpu.make_async_copy(w_hbm.at[:, pl.ds(0, 3)], w_s, w_sem)

        def add0(wave):
            to_core(wave).wait()
            if wave == 0:
                mine_of_out().wait()
            for k, part in enumerate(PARTS):
                dims = _order(wave, k)
                b = bits[dims[0]]

                def pair(i):
                    second, third = i // 2, i % 2

                    def total(first):
                        p = at(dims, first, second, third)
                        return g_s[(slot[wave], *p, core, ALL, part)].astype(F32) + r0_s[(wave, *p, ALL, part)].astype(F32)

                    s1[k][wave, second, third] = total(1 - b).astype(BF16)
                    a_s[k][wave, second, third] = total(b)

                _loop(4, pair)
            for k in WAYS:
                hop(wave, k, 0).start()

        def add1(wave):
            for k in WAYS:
                hop(wave, k, 0).wait_recv()
                b = bits[_order(wave, k)[1]]

                def one(third):
                    s2[k][wave, third] = (a_s[k][wave, 1 - b, third] + r1[k][wave, 1 - b, third].astype(F32)).astype(BF16)
                    a_s[k][wave, b, third] = a_s[k][wave, b, third] + r1[k][wave, b, third].astype(F32)

                _loop(2, one)
            for k in WAYS:
                hop(wave, k, 1).start()

        def add2(wave):
            for k in WAYS:
                hop(wave, k, 1).wait_recv()
                dims = _order(wave, k)
                b, c = bits[dims[1]], bits[dims[2]]
                s3[k][wave] = (a_s[k][wave, b, 1 - c] + r2[k][wave, 1 - c].astype(F32)).astype(BF16)
                a_s[k][wave, b, c] = a_s[k][wave, b, c] + r2[k][wave, c].astype(F32)
            for k in WAYS:
                hop(wave, k, 2).start()

        def add3(wave):
            for k, part in enumerate(PARTS):
                hop(wave, k, 2).wait_recv()
                dims = _order(wave, k)
                b, c = bits[dims[1]], bits[dims[2]]
                sum_ref[(wave + len(WAYS)) % waves, :, part] = (a_s[k][wave, b, c] + r3[k][wave].astype(F32)).astype(BF16)

        @pl.when(t == 0)
        def _():
            _meet((other, *across))
            to_core(0).start()
            mine_of_out().start()
            weights().start()

        @pl.when(t < makes)
        def _():
            made = _tn(a_ref[:], d_col[0]).astype(BF16).reshape(*TORUS, rows, bn)
            g_s[(t // tiles) % 2, :, :, :, :, :, pl.ds(pl.multiple_of(t % tiles * bn, bn), bn)] = made

        @pl.when(t == makes)
        def _():
            weights().wait()

        @pl.when(t >= makes)
        def _():
            part = sum(_nt(d_row[m], w_s[:, m].reshape(dim, width)) for m in range(3))
            o_ref[:] = _through_norm(h_ref[:], part, y_ref[:])

        last = makes + backs - 1
        plan = {add0: (3, 9, 14, 16), add1: (12, 18, 18, 19), add2: (16, 20, 20, 21), add3: (18, last, last, last)}
        for action, times in plan.items():
            for wave, step in enumerate(times):
                pl.when(t == step)(functools.partial(action, wave))
        for wave in range(1, waves):
            pl.when(t == tiles * wave - 1)(functools.partial(lambda i: to_core(i).start(), wave))

        @pl.when(t == last)
        def _():
            for wave in range(waves):
                for stage in WAYS:
                    for k in WAYS:
                        hop(wave, k, stage).wait_send()

    def made(t):
        return jnp.minimum(t, makes - 1)

    def back(t):
        return jnp.maximum(t - makes, 0)

    wide = [part.stop - part.start for part in PARTS]
    tile = lambda t: (back(t), 0)
    total, summed = pl.pallas_call(
        body,
        grid=(makes + backs,),
        in_specs=[
            pl.BlockSpec((1, s, bn), lambda t: (made(t) // tiles, 0, made(t) % tiles)), _spec((s, dim), _FLAT),
            pl.BlockSpec((3, bm, width), lambda t: (0, back(t), 0)), pl.BlockSpec((bm, dim), tile), pl.BlockSpec((bm, dim), tile),
            ANY, ANY,
        ],
        out_specs=[pl.BlockSpec((bm, dim), tile), pl.BlockSpec((waves, rows, width), _CUBE)],
        out_shape=[_shape((s, dim)), _shape((waves, rows, width))],
        scratch_shapes=[
            pltpu.VMEM((n, 3, rows, width), BF16), pltpu.VMEM((2, *TORUS, rows, width), BF16), pltpu.VMEM((waves, *TORUS[1:], rows, width), BF16),
            *(pltpu.VMEM((waves, 2, 2, rows, x), F32) for x in wide),
            *(pltpu.VMEM((waves, *((2,) * (2 - i)), rows, x), BF16) for i in WAYS for _ in range(2) for x in wide),
            pltpu.SemaphoreType.DMA, pltpu.SemaphoreType.DMA, *_link_sems(waves),
        ],
        compiler_params=pltpu.CompilerParams(vmem_limit_bytes=VMEM, dimension_semantics=("arbitrary",), collective_id=0, has_side_effects=True),
        cost_estimate=pl.CostEstimate(flops=12 * s * dim * width, bytes_accessed=60 * 2**20, transcendentals=0),
    )(d, a, d, h, by_h, w, g_out.reshape(*TORUS, rows, width))
    return total, summed


def collect(y, qkvo, gu, dn):
    layers, (s, d), (_, _, rows, third) = len(dn), y.shape, gu[0].shape
    ff = len(WAYS) * third
    shapes = [_shape(y.shape), *[_shape((layers, rows, d))] * 4, *[_shape((layers, rows, ff))] * 2, _shape((layers, *dn[0].shape))]
    parts = [y, *qkvo, *gu, *dn]

    def moves(l):
        if l < 0:
            return [(0, (here,), 0, (here,)) for here in _cuts(s, 512)]
        at = range(l + 1, len(parts), layers)
        return [
            *((at[0], (here,), i + 1, (l,)) for i, here in enumerate(_cuts(4 * rows, rows))),
            *((at[1], (k, i), 5 + i, (l, ALL, here)) for i in (0, 1) for k, here in enumerate(_cuts(ff, third))),
            (at[2], (), 7, (l,)),
        ]

    plan = [move for l in range(-1, layers) for move in moves(l)]

    def body(*refs):
        from_, to, held, came, left = refs[: len(parts)], refs[len(parts) :][: len(shapes)], refs[len(parts) + len(shapes) : -2], refs[-2], refs[-1]

        def bring(i):
            part, place, _, _ = plan[i]
            return pltpu.make_async_copy(from_[part].at[place], held[part].at[place], came.at[i])

        def put(i):
            part, place, out, target = plan[i]
            return pltpu.make_async_copy(held[part].at[place], to[out].at[target], left.at[i])

        for i in range(len(plan)):
            bring(i).start()
        for i in range(len(plan)):
            bring(i).wait()
            put(i).start()
        for i in range(len(plan)):
            put(i).wait()

    sems = [pltpu.SemaphoreType.DMA((len(plan),))] * 2
    any_ = (None, None)
    return _call(body, (1,), [any_] * len(parts), [any_] * len(shapes), shapes, s, parts, [*(pltpu.VMEM(x.shape, BF16) for x in parts), *sems])


def solution(mesh):
    n = mesh.shape["dp"]

    def gather(t):
        return lax.all_gather(t, "dp", axis=0, tiled=True)

    def scatter(t):
        flat = lax.psum_scatter(t.reshape(-1, t.shape[-1]), "dp", scatter_dimension=0, tiled=True)
        return flat.reshape(t.shape[1:])

    def step(x, dy, wq, wk, wv, wo, w_gate, w_up, w_down):
        layers, rows, width = wq.shape
        ff = w_gate.shape[2]
        s = x.shape[1]
        cos, sin = _tables(s)
        h = x[0]
        kept = []
        for l in range(layers):
            if l:
                w_qkvo, w_gu = (gather(x).reshape(n, -1, rows, x.shape[-1]) for x in packed)
                w_out, w_dn = w_qkvo, gather(w_down[l])
                qkv = project(a, w_qkvo, cos, sin)
            else:
                w_out = gather(wo[l]).reshape(n, -1, rows, width)
                w_gu = gather(jnp.concatenate([w_gate[l], w_up[l]], axis=0)).reshape(n, -1, rows, ff)
                a, qkv, w_qkvo, packed = fetch_and_project(h, cos, sin, (wq, wk, wv), ((wq, wk, wv, wo), (w_gate, w_up)))
            out, lse = attend(qkv)
            mid, b = add_matmul(out, w_out, h, (n, 1, rows, width), (0, w_out.shape[1] - 1, 0, 0))
            g, u, act, *carried = gate_up(b, w_gu, None if l else _Carry(w_down, 2))
            w_dn = w_dn if l else carried[0].reshape(-1, w_down.shape[-1])
            kept.append((w_qkvo, w_out, w_gu, w_dn, h, a, qkv, out, lse, mid, b, g, u, act))
            if l + 1 < layers:
                h, a = add_matmul(act, w_dn, mid)

        y = dy[0]
        of = []
        for l in reversed(range(layers)):
            w_qkvo, w_out, w_gu, w_dn, h, a, qkv, out, lse, mid, b, g, u, act = kept[l]
            dg, du, g_dn, g_gu = mlp_back(y, w_dn, g, u, act, b, n)
            of_gu = scatter(g_gu)
            of_dn = scatter(g_dn.reshape(n, -1, g_dn.shape[1]))
            y_mid = back_gate_up(dg, du, w_gu, mid, y)
            if l == 0:
                g_out, y_mid = after(grad_out(out, y_mid, n), y_mid)
            d = attend_back(qkv, out, lse, back_out(y_mid, w_out), cos, sin)
            if l == 0:
                y, of_qkvo = back_project_and_sum(a, d, g_out, w_qkvo, h, y_mid)
                of.append((of_qkvo.reshape(-1, width), of_gu, of_dn))
                break
            g_qkvo, d = after(grad_project(a, d, out, y_mid, n), d)
            of_qkvo = scatter(g_qkvo)
            y = back_project(d, w_qkvo, h, y_mid)
            of.append((of_qkvo, of_gu, of_dn))
        y, *rest = collect(y, *zip(*reversed(of)))
        return y[None], *rest

    states, cut = P(("rep", "dp"), None, None), P(None, "dp", None)
    return jax.shard_map(
        step,
        mesh=mesh,
        in_specs=(states, states) + (cut,) * 7,
        out_specs=(states,) + (P("rep", "dp", None),) * 7,
        check_vma=False,
    )
```

```python
import functools

import jax
import jax.numpy as jnp
import numpy as np
from jax import lax
from jax.experimental import pallas as pl
from jax.experimental.pallas import tpu as pltpu
from jax.sharding import PartitionSpec as P


HEAD = 128
THETA = 10000
EPS = 1e-6
LOG2E = 1.4426950408889634
HIDDEN = -2e30
LOW = -1e30
VMEM = 63 * 2**20
BF16, F32 = jnp.bfloat16, jnp.float32


def _dot(a, b, ca, cb):
    return lax.dot_general(a, b, (((ca,), (cb,)), ((), ())), preferred_element_type=F32)


def _nn(a, b):
    return _dot(a, b, 1, 0)


def _nt(a, b):
    return _dot(a, b, 1, 1)


def _tn(a, b):
    return _dot(a, b, 0, 0)


def _row(i):
    return i, 0


def _col(i):
    return 0, i


class _fixed:
    def __init__(self, rank, *last):
        self.place = (0,) * (rank - len(last)) + last

    def __call__(self, *_):
        return self.place


def _spec(block, index):
    if block is None:
        return ANY
    return pl.BlockSpec(block, index, pipeline_mode=pl.Buffered(1)) if isinstance(index, _fixed) else pl.BlockSpec(block, index)


def _step():
    return pl.program_id(0)


def _cuts(size, step):
    return [slice(x, min(x + step, size)) for x in range(0, size, step)]


def _loop(count, body):
    lax.fori_loop(0, count, lambda i, _: body(i), None)


_FLAT, _CUBE, _QUAD = _fixed(2), _fixed(3), _fixed(4)


def _call(body, grid, ins, outs, shapes, work, args, scratch=(), carry=None):
    moved = sum(a.size * a.dtype.itemsize for a in (*args, *shapes))
    params = {"vmem_limit_bytes": VMEM, "dimension_semantics": ("arbitrary",) * len(grid)}
    ins, outs, shapes, args, scratch = [_spec(*x) for x in ins], [_spec(*x) for x in outs], list(shapes), list(args), list(scratch)
    if carry:
        body = carry.beside(body, len(ins), len(outs))
        ins, args, outs, shapes, scratch = [*ins, ANY], [*args, carry.shard], [*outs, ANY], [*shapes, carry.shape()], [*carry.scratch(), *scratch]
        params |= {"collective_id": carry.number, "has_side_effects": True}
    results = pl.pallas_call(
        body,
        grid=grid,
        in_specs=ins,
        out_specs=outs,
        out_shape=shapes,
        scratch_shapes=scratch,
        compiler_params=pltpu.CompilerParams(**params),
        cost_estimate=pl.CostEstimate(flops=2 * work, bytes_accessed=moved, transcendentals=0),
    )(*args)
    return results if len(shapes) > 1 else results[0]


def _shape(shape, dtype=BF16):
    return jax.ShapeDtypeStruct(shape, dtype)


def _scale(wide):
    return lax.rsqrt(jnp.mean(wide * wide, -1, keepdims=True) + EPS)


def _sum_and_normed(h, part):
    total = (h.astype(F32) + part.astype(BF16).astype(F32)).astype(BF16)
    wide = total.astype(F32)
    return total, (wide * _scale(wide)).astype(BF16)


def _through_norm(h, by_b, by_h):
    wide, c = h.astype(F32), by_b.astype(BF16).astype(F32)
    r = _scale(wide)
    along = jnp.sum(c * wide, -1, keepdims=True)
    part = (c * r - wide * (along * (r * r * r) / wide.shape[-1])).astype(BF16)
    return (by_h.astype(F32) + part.astype(F32)).astype(BF16)


def _turn(t, cos, sin):
    x = t.astype(F32)
    return (x * cos + pltpu.roll(x, HEAD // 2, 1) * sin).astype(BF16)


def _turn_back(t, cos, sin):
    x = t.astype(BF16).astype(F32)
    return (x * cos - pltpu.roll(x, HEAD // 2, 1) * sin).astype(BF16)


PARTS = (slice(0, 384), slice(384, 768), slice(768, 1280))
ANY = pl.BlockSpec(memory_space=pl.ANY)
TORUS = (2, 2, 2, 2)
WAYS = range(3)
PAIR = range(2)
ALL = slice(None)


def _here():
    me = lax.axis_index("dp")
    bits = [me // 8, me // 4 % 2, me // 2 % 2]
    core = me % 2
    return bits, core, me + 1 - 2 * core, [me + far * (1 - 2 * b) for far, b in zip((8, 4, 2), bits)]


def _order(wave, k):
    return [(k + wave + i) % 3 for i in WAYS]


def _send(source, target, sent, came, device):
    return pltpu.make_async_remote_copy(
        src_ref=source, dst_ref=target, send_sem=sent, recv_sem=came, device_id={"dp": device}, device_id_type=pl.DeviceIdType.MESH
    )


def _meet(devices):
    barrier = pltpu.get_barrier_semaphore()
    for device in devices:
        pl.semaphore_signal(barrier, inc=1, device_id={"dp": device}, device_id_type=pl.DeviceIdType.MESH)
    pl.semaphore_wait(barrier, len(devices))


def _link_sems(waves):
    return [pltpu.SemaphoreType.DMA((waves, 3, 3))] * 2 + [pltpu.SemaphoreType.DMA((waves,))] * 2


class _Spread:
    def __init__(self, own, whole, pick, sems):
        self.own, self.whole, self.pick = own, whole, pick
        self.sent, self.came, self.core_sent, self.core_came, self.stored = sems
        self.bits, self.core, self.other, self.across = _here()

    def _hop(self, wave, stage, k):
        dims = _order(wave, k)
        place = [ALL if i in dims[:stage] else b for i, b in enumerate(self.bits)]
        target = self.whole.at[(*place, self.core, *self.pick[wave], PARTS[k])]
        source = target if stage else self.own.at[(*self.pick[wave], PARTS[k])]
        return _send(source, target, self.sent.at[wave, stage, k], self.came.at[wave, stage, k], self.across[dims[stage]])

    def _to_core(self, wave):
        mine = self.whole.at[(*[ALL] * 3, self.core, *self.pick[wave])]
        return _send(mine, mine, self.core_sent.at[wave], self.core_came.at[wave], self.other)

    def _store(self, wave):
        return pltpu.make_async_copy(self.own.at[self.pick[wave]], self.whole.at[(*self.bits, self.core, *self.pick[wave])], self.stored.at[wave])

    def start(self, wave, stage=0):
        for k in WAYS:
            if stage:
                self._hop(wave, stage - 1, k).wait_recv()
        if stage == 1:
            self._store(wave).wait()
        for k in WAYS:
            if stage < 3:
                self._hop(wave, stage, k).start()
        if stage == 0:
            self._store(wave).start()
        if stage == 3:
            self._to_core(wave).start()

    def finish(self, wave):
        self._to_core(wave).wait()
        for stage in WAYS:
            for k in WAYS:
                self._hop(wave, stage, k).wait_send()


class _Carry:
    def __init__(self, shard, number, depth):
        self.shard, self.number, self.block = shard, number, shard.shape[1:]
        self.pick = [(rows,) for rows in _cuts(self.block[0], depth)]

    def shape(self):
        return _shape((*TORUS, *self.block))

    def scratch(self):
        waves = len(self.pick)
        return [pltpu.VMEM(self.block, BF16), pltpu.SemaphoreType.DMA, *_link_sems(waves), pltpu.SemaphoreType.DMA((waves,))]

    def beside(self, body, n_in, n_out):
        count = len(self.scratch())

        def both(*refs):
            t = _step()
            shard, outs, (whole, own_s, own_sem, *rest) = refs[n_in], refs[n_in + 1 :][:n_out], refs[n_in + 1 + n_out :]
            sems, scratch = rest[: count - 2], rest[count - 2 :]
            spread = _Spread(own_s, whole, self.pick, sems)

            @pl.when(t == 0)
            def _():
                own = pltpu.make_async_copy(shard.at[0], own_s, own_sem)
                own.start()
                _meet((spread.other, *spread.across))
                own.wait()
                for wave in range(len(self.pick)):
                    spread.start(wave)

            body(*refs[:n_in], *outs, *scratch)
            for stage in WAYS:
                for wave in range(len(self.pick)):
                    pl.when(t == wave + 2 * stage)(functools.partial(spread.start, wave, stage + 1))

            @pl.when(t == pl.num_programs(0) - 1)
            def _():
                for wave in range(len(self.pick)):
                    spread.finish(wave)

        return both


def fetch_and_project(x, cos, sin, shards, packs):
    (s, d), (_, rows, width) = x.shape, shards[0].shape
    n, waves, bm, sub = 16, len(shards), s // 2, 256
    loose = [x for pack in packs for x in pack]
    packed = [_shape((len(pack) * pack[0].shape[1], pack[0].shape[2])) for pack in packs]

    def body(x_hbm, c_ref, s_ref, *rest):
        parts, rest = rest[:waves], rest[waves:]
        loose_, rest = rest[: len(loose)], rest[len(loose) :]
        (a_ref, o_ref, whole), packed_, rest = rest[:3], rest[3 : 3 + len(packs)], rest[3 + len(packs) :]
        held, (own_s, x_s, w_s, own_sem, x_sem, w_sem, came, left), sems = rest[: len(packs)], rest[len(packs) : -5], rest[-5:]
        t = _step()
        spread = _Spread(own_s, whole, [(i, ALL) for i in range(waves)], sems)

        def own(i):
            return pltpu.make_async_copy(parts[i].at[0], own_s.at[i], own_sem.at[i])

        def states():
            return pltpu.make_async_copy(x_hbm, x_s, x_sem)

        def weights(i):
            return pltpu.make_async_copy(whole.at[(*[ALL] * len(TORUS), i)], w_s.at[i % 2], w_sem)

        def bring():
            of = [(k, i) for k, pack in enumerate(packs) for i in range(len(pack))]
            rows_ = [pack[0].shape[1] for pack in packs]
            return [
                pltpu.make_async_copy(loose_[j].at[1], held[k].at[pl.ds(i * rows_[k], rows_[k])], came.at[j]) for j, (k, i) in enumerate(of)
            ]

        def put():
            return [pltpu.make_async_copy(held[k], packed_[k], left.at[k]) for k in range(len(packs))]

        def ready(i):
            spread.finish(i)
            weights(i).start()
            weights(i).wait()

        def begin():
            for i in range(waves):
                own(i).start()
            states().start()
            _meet((spread.other, *spread.across))
            for i in range(waves):
                own(i).wait()
                spread.start(i)
            states().wait()

            def norm(i):
                here = pl.ds(pl.multiple_of(i * sub, sub), sub)
                wide = x_s[here, :].astype(F32)
                a_ref[here, :] = (wide * _scale(wide)).astype(BF16)

            for copy in bring():
                copy.start()
            quarter = s // sub // 4
            for part, wave in enumerate((None, 0, 1, None)):
                _loop(quarter, lambda i: norm(part * quarter + i))
                if wave is not None:
                    spread.start(wave, 1)
            for copy in bring():
                copy.wait()
            for copy in put():
                copy.start()
            spread.start(0, 2)
            spread.start(2, 1)
            spread.start(1, 2)
            spread.start(0, 3)
            for copy in put():
                copy.wait()
            ready(0)

        pl.when(t == 0)(begin)

        def run(turn, matrix, half):
            ww = w_s[matrix % 2].reshape(d, width)
            for r in range(0, bm, sub):
                here = pl.ds(pl.multiple_of(half * bm + r, sub), sub)
                y = _nn(a_ref[here, :], ww).astype(BF16)
                if turn:
                    c, sn = c_ref[here, :], s_ref[here, :]
                    for k in range(0, width, HEAD):
                        o_ref[0, r : r + sub, k : k + HEAD] = _turn(y[:, k : k + HEAD], c, sn)
                else:
                    o_ref[0, r : r + sub, :] = y

        matrix, half = (t - 1) // 2, (t + 1) % 2
        pl.when((t > 0) & (matrix < 2))(lambda: run(True, matrix, half))
        pl.when(matrix == 2)(lambda: run(False, matrix, half))
        after_step = (), ((spread.start, 2, 2), (spread.start, 1, 3)), ((ready, 1),), ((spread.start, 2, 3),), ((ready, 2),)
        for step, actions in enumerate(after_step):

            @pl.when(t == step)
            def _():
                for action, *args in actions:
                    action(*args)

    def at(t):
        return jnp.maximum(t - 1, 0)

    a, qkv, whole, *packed = pl.pallas_call(
        body,
        grid=(7,),
        in_specs=[ANY, *[_spec((s, HEAD), _FLAT)] * 2, *[ANY] * (waves + len(loose))],
        out_specs=[pl.BlockSpec((s, d), _FLAT), pl.BlockSpec((1, bm, width), lambda t: (at(t) // 2, at(t) % 2, 0)), *[ANY] * (1 + len(packs))],
        out_shape=[_shape((s, d)), _shape((3, s, width)), _shape((*TORUS, waves, rows, width)), *packed],
        scratch_shapes=[
            *(pltpu.VMEM(x.shape, BF16) for x in packed),
            pltpu.VMEM((waves, rows, width), BF16), pltpu.VMEM((s, d), BF16), pltpu.VMEM((2, *TORUS, rows, width), BF16),
            pltpu.SemaphoreType.DMA((waves,)), pltpu.SemaphoreType.DMA, pltpu.SemaphoreType.DMA,
            pltpu.SemaphoreType.DMA((len(loose),)), pltpu.SemaphoreType.DMA((len(packs),)), *_link_sems(waves), pltpu.SemaphoreType.DMA((waves,)),
        ],
        compiler_params=pltpu.CompilerParams(vmem_limit_bytes=VMEM, collective_id=1, has_side_effects=True),
        cost_estimate=pl.CostEstimate(flops=12 * s * d * width, bytes_accessed=VMEM, transcendentals=0),
    )(x, cos, sin, *shards, *loose)
    return a, qkv, whole.reshape(n, waves, rows, width), packed


def project(a, w, cos, sin):
    (s, d), (n, _, rows, width) = a.shape, w.shape
    bm, sub = min(1024, s), 256

    def body(a_ref, w_ref, c_ref, s_ref, o_ref):
        which, at = _step(), pl.program_id(1)
        ww = w_ref[:].reshape(d, width)

        def run(turn):
            for r in range(0, bm, sub):
                t = _nn(a_ref[r : r + sub, :], ww).astype(BF16)
                if turn:
                    here = pl.ds(at * bm + r, sub)
                    c, sn = c_ref[here, :], s_ref[here, :]
                    for x in range(0, width, HEAD):
                        o_ref[0, r : r + sub, x : x + HEAD] = _turn(t[:, x : x + HEAD], c, sn)
                else:
                    o_ref[0, r : r + sub, :] = t

        pl.when(which < 2)(lambda: run(True))
        pl.when(which == 2)(lambda: run(False))

    return _call(
        body, (3, s // bm),
        [((bm, d), lambda m, i: (i, 0)), ((n, 1, rows, width), lambda m, i: (0, m, 0, 0)), ((s, HEAD), _FLAT), ((s, HEAD), _FLAT)],
        [((1, bm, width), lambda m, i: (m, i, 0))], [_shape((3, s, width))], 3 * s * d * width, (a, w, cos, sin),
    )


def _seen(keys, queries):
    place = [lax.broadcasted_iota(jnp.int32, (keys, queries), i) for i in PAIR]
    return place[1] >= place[0]


def _heads(b, s, hb):
    return [((1, b, hb * HEAD), lambda g, i: (0, i, g)), *(((1, s, hb * HEAD), lambda g, i, m=m: (m, 0, g)) for m in (1, 2))]


def _few(b, hb):
    return (b, hb * HEAD), lambda g, i: (i, g)


def _stats(b, hb):
    return (1, hb, b), lambda g, i: (g, 0, i)


def attend(qkv):
    _, s, width = qkv.shape
    heads = width // HEAD
    hb, b = 5, 512
    half = b // 2
    e = HEAD**-0.5 * LOG2E

    def body(q_ref, k_ref, v_ref, o_ref, lse_ref, top_s, mix_s):
        iq = pl.program_id(1)
        cols = [slice(i * HEAD, (i + 1) * HEAD) for i in range(hb)]
        top_s[:] = jnp.full(top_s.shape, LOW, F32)
        mix_s[:] = jnp.zeros(mix_s.shape, F32)

        def block(j, nk, rows, diagonal):
            here = pl.ds(j, nk)
            ones = jnp.ones((8, nk), BF16)
            scores = [_nt(k_ref[0, here, c], q_ref[0, rows, c]) for c in cols]
            if diagonal:
                seen = _seen(nk, len(range(b)[rows]))
            weights, keeps = [], []
            for i, x in enumerate(scores):
                if diagonal:
                    x = jnp.where(seen, x, HIDDEN)
                old = top_s[i : i + 1, rows]
                top = jnp.maximum(old, x.max(axis=0, keepdims=True))
                top_s[i : i + 1, rows] = top
                weights.append(jnp.exp2((x - top) * e).astype(BF16))
                keeps.append(jnp.exp2((old - top) * e))
            for i, (c, p, keep) in enumerate(zip(cols, weights, keeps)):
                values = jnp.concatenate([v_ref[0, here, c].T, ones])
                mix_s[i, :, rows] = mix_s[i, :, rows] * keep + _nn(values, p)

        base = pl.multiple_of(iq * b, b)
        _loop(iq, lambda j: block(pl.multiple_of(j * b, b), b, slice(b), False))
        block(base, half, slice(b), True)
        block(base + half, half, slice(half, b), True)
        for i, c in enumerate(cols):
            total = mix_s[i, HEAD : HEAD + 1, :]
            o_ref[:, c] = (mix_s[i, :HEAD, :] * (1 / total)).T.astype(BF16)
            lse_ref[0, i : i + 1, :] = top_s[i : i + 1, :] * e + jnp.log2(total)

    return _call(
        body, (heads // hb, s // b), _heads(b, s, hb), [_few(b, hb), _stats(b, hb)],
        [_shape((s, width)), _shape((heads // hb, hb, s), F32)], s * s * width, (qkv, qkv, qkv),
        [pltpu.VMEM((hb, b), F32), pltpu.VMEM((hb, HEAD + 8, b), F32)],
    )


def add_matmul(a, w, h, block=None, at=None):
    s, d, width = a.shape[0], a.shape[1], h.shape[1]
    bm, sub = 512, 256
    block, at = block or w.shape, at or (0,) * w.ndim

    def body(a_ref, w_ref, h_ref, o_ref, b_ref):
        ww = w_ref[:].reshape(d, width)
        for here in _cuts(bm, sub):
            o_ref[here, :], b_ref[here, :] = _sum_and_normed(h_ref[here, :], _nn(a_ref[here, :], ww))

    return _call(
        body, (s // bm,), [((bm, d), _row), (block, _fixed(len(at), *at)), ((bm, width), _row)], [((bm, width), _row)] * 2,
        [_shape((s, width))] * 2, s * d * width, (a, w, h),
    )


def gate_up(b, w, carry=None):
    (s, d), (n, _, rows, ff) = b.shape, w.shape
    bn, sub = 384, 256

    def body(b_ref, w_ref, g_ref, u_ref, act_ref):
        ww = jnp.concatenate([w_ref[:, 0].reshape(d, bn), w_ref[:, 1].reshape(d, bn)], axis=1)
        for here in _cuts(s, sub):
            t = _nn(b_ref[here, :], ww)
            g, u = t[:, :bn], t[:, bn:]
            g_ref[here, :] = g
            u_ref[here, :] = u
            act_ref[here, :] = (g * jax.nn.sigmoid(g) * u).astype(BF16)

    return _call(
        body, (ff // bn,), [((s, d), _FLAT), ((n, 2, rows, bn), lambda i: (0, 0, 0, i))], [((s, bn), _col)] * 3,
        [_shape((s, ff), F32), _shape((s, ff), F32), _shape((s, ff))], 2 * s * d * ff, (b, w), carry=carry,
    )


def _sum_as_loaded(load, product, count, finish, rest=None):
    @pl.when(_step() == 0)
    def _():
        for i in range(count):
            load(i).start()
        part = None
        for i in range(count):
            load(i).wait()
            part = product(i) if part is None else part + product(i)
        finish(part)

    @pl.when(_step() > 0)
    def _():
        finish(rest() if rest else sum(map(product, range(count))))


def back_gate_up(dg, du, w, h, by_h):
    (s, ff), d = dg.shape, h.shape[1]
    bm = 256
    cuts = _cuts(ff, d)
    parts = [(i, c) for i in PAIR for c in cuts]

    def body(dg_ref, du_ref, w_hbm, h_ref, y_ref, o_ref, w_s, sem):
        both = dg_ref, du_ref

        def load(k):
            i, c = parts[k]
            return pltpu.make_async_copy(w_hbm.at[:, i, :, c], w_s.at[:, i, :, c], sem.at[k])

        def product(k):
            i, c = parts[k]
            return _nt(both[i][:, c], w_s[:, i, :, c].reshape(d, -1))

        def finish(part):
            o_ref[:] = _through_norm(h_ref[:], part, y_ref[:])

        _sum_as_loaded(load, product, len(parts), finish, lambda: sum(_nt(x[:], w_s[:, i].reshape(d, ff)) for i, x in enumerate(both)))

    return _call(
        body, (s // bm,), [((bm, ff), _row), ((bm, ff), _row), (None, None), ((bm, d), _row), ((bm, d), _row)], [((bm, d), _row)],
        [_shape((s, d))], 2 * s * d * ff, (dg, du, w, h, by_h), [pltpu.VMEM(w.shape, BF16), pltpu.SemaphoreType.DMA((len(parts),))],
    )


def attend_back(qkv, out, lse, by_mid, w, cos, sin):
    (_, s, width), (n, parts, rows_, dim) = qkv.shape, w.shape
    groups, hb, _ = lse.shape
    b = 512
    half = b // 2
    scale = HEAD**-0.5
    e = scale * LOG2E

    def body(q_ref, k_ref, v_ref, o_ref, m_ref, w_ref, lse_ref, c_ref, s_ref, d_ref, dq_s, dk_s, dv_s, t_s, y_s):
        iq = pl.program_id(1)
        cols = [slice(i * HEAD, (i + 1) * HEAD) for i in range(hb)]
        base = pl.multiple_of(iq * b, b)

        def block(j, nk, rows, diagonal):
            here = pl.ds(j, nk)
            scores = [_nt(k_ref[0, here, c], q_ref[0, rows, c]) for c in cols]
            dps = [_nt(v_ref[0, here, c], y_s[rows, c]) for c in cols]
            if diagonal:
                seen = _seen(nk, len(range(b)[rows]))
            for i, c in enumerate(cols):
                p = jnp.exp2(scores[i] * e - lse_ref[0, i : i + 1, rows])
                if diagonal:
                    p = jnp.where(seen, p, 0.0)
                ds = (p * (dps[i] - t_s[i : i + 1, rows])).astype(BF16)
                dv = _nn(p.astype(BF16), y_s[rows, c])
                dk = _nn(ds, q_ref[0, rows, c])
                dv_s[i, here, :] = dv if diagonal else dv_s[i, here, :] + dv
                dk_s[i, here, :] = dk if diagonal else dk_s[i, here, :] + dk
                dq_s[i, :, rows] += _nn(k_ref[0, here, c].T, ds)

        y_s[:] = _nt(m_ref[:], w_ref[:].reshape(-1, dim)).astype(BF16)
        for i, c in enumerate(cols):
            t_s[i : i + 1, :] = (y_s[:, c].astype(F32) * o_ref[:, c].astype(F32)).T.sum(axis=0, keepdims=True)
        dq_s[:] = jnp.zeros_like(dq_s)
        block(base, half, slice(b), True)
        block(base + half, half, slice(half, b), True)
        _loop(iq, lambda j: block(pl.multiple_of(j * b, b), b, slice(b), False))
        here = pl.ds(base, b)
        for i, c in enumerate(cols):
            d_ref[0, here, c] = _turn_back((dq_s[i] * scale).T, c_ref[here, :], s_ref[here, :])

        @pl.when(iq == pl.num_programs(1) - 1)
        def _():
            def finish(j):
                rows = pl.ds(pl.multiple_of(j * b, b), b)
                for i, c in enumerate(cols):
                    d_ref[1, rows, c] = _turn_back(dk_s[i, rows, :] * scale, c_ref[rows, :], s_ref[rows, :])
                    d_ref[2, rows, c] = dv_s[i, rows, :].astype(BF16)

            _loop(s // b, finish)

    return _call(
        body, (groups, s // b),
        [*_heads(b, s, hb), _few(b, hb), ((b, dim), lambda g, i: (i, 0)), ((n // groups, 1, rows_, dim), lambda g, i: (g, parts - 1, 0, 0)),
         _stats(b, hb), ((s, HEAD), _FLAT), ((s, HEAD), _FLAT)],
        [((3, s, hb * HEAD), lambda g, i: (0, 0, g))], [_shape((3, s, width))], 3 * s * s * width, (qkv, qkv, qkv, out, by_mid, w, lse, cos, sin),
        [pltpu.VMEM((hb, HEAD, b), F32), pltpu.VMEM((hb, s, HEAD), F32), pltpu.VMEM((hb, s, HEAD), F32), pltpu.VMEM((hb, b), F32), pltpu.VMEM((b, hb * HEAD), BF16)],
    )


def back_project(d, w, h, by_h):
    (_, s, width), n, rows = d.shape, w.shape[0], w.shape[2]
    dim = h.shape[1]
    bm = 256

    def body(d_ref, w_ref, h_ref, y_ref, o_ref):
        part = sum(_nt(d_ref[m], w_ref[:, m].reshape(dim, width)) for m in range(3))
        o_ref[:] = _through_norm(h_ref[:], part, y_ref[:])

    return _call(
        body, (s // bm,), [((3, bm, width), lambda i: (0, i, 0)), ((n, 3, rows, width), _QUAD), ((bm, dim), _row), ((bm, dim), _row)],
        [((bm, dim), _row)], [_shape((s, dim))], 3 * s * dim * width, (d, w, h, by_h),
    )


def grad_project(a, d, out, by_mid, n):
    (s, dim), width = a.shape, d.shape[2]
    rows, bn = dim // n, 256
    padded = -(-4 * rows // 24) * 24

    def body(a_ref, d_ref, out_ref, m_ref, o_ref):
        which = _step()

        @pl.when(which < 3)
        def _():
            o_ref[:] = _tn(a_ref[:], d_ref[0]).astype(BF16).reshape(n, rows, bn)

        @pl.when(which == 3)
        def _():
            o_ref[:] = _tn(out_ref[:], m_ref[:]).astype(BF16).reshape(n, rows, bn)

    last = width // bn - 1
    return _call(
        body, (4, width // bn),
        [((s, dim), _FLAT), ((1, s, bn), lambda m, i: (jnp.minimum(m, 2), 0, jnp.where(m < 3, i, last))),
         ((s, width), _FLAT), ((s, bn), lambda m, i: (0, jnp.where(m < 3, 0, i)))],
        [((n, rows, bn), lambda m, i: (0, m, i))], [_shape((n, padded, width))], 4 * s * dim * width, (a, d, out, by_mid),
    )


def grad_out(out, by_mid, n):
    (s, width), d = out.shape, by_mid.shape[1]
    rows, bn = width // n, 256

    def body(out_ref, m_ref, o_ref):
        o_ref[:] = _tn(out_ref[:], m_ref[:]).astype(BF16).reshape(n, rows, bn)

    return _call(
        body, (d // bn,), [((s, width), _FLAT), ((s, bn), _col)], [((n, rows, bn), lambda i: (0, 0, i))], [_shape((n, rows, d))],
        s * d * width, (out, by_mid),
    )


def mlp_back(y, w, g, u, act, b, n):
    (s, d), ff = y.shape, w.shape[0]
    rows, bn, third, sub = d // n, 384, ff // 3, 512
    per = third // bn

    tiles = ff // bn

    def body(y_ref, w_ref, g_ref, u_ref, act_ref, b_ref, dg_ref, du_ref, dn_ref, gu_ref, t_s):
        at = _step()

        def turn(here, t):
            t = t.astype(F32)
            gate, up = g_ref[here, :], u_ref[here, :]
            sig = jax.nn.sigmoid(gate)
            part = sig * t
            du_ref[here, :] = (part * gate).astype(BF16)
            dg_ref[here, :] = (part * up * (1 + gate * (1 - sig))).astype(BF16)

        def down():
            dn_ref[:] = _tn(act_ref[:], y_ref[:]).astype(BF16)

        def gate_up_():
            both = jnp.concatenate([dg_ref[:], du_ref[:]], axis=1)
            for them in _cuts(n, n // 4):
                t = _tn(b_ref[:, them.start * rows : them.stop * rows], both).astype(BF16)
                for i in PAIR:
                    gu_ref[them, 0, i] = t[:, i * bn :][:, :bn].reshape(-1, rows, bn)

        @pl.when((at % 2 == 0) & (at < tiles - 1))
        def _():
            for here in _cuts(s, sub):
                t = _nt(y_ref[here, :], w_ref[:]).astype(BF16)
                turn(here, t[:, :bn])
                t_s[here, :] = t[:, bn:]
            down()
            gate_up_()

        @pl.when(at % 2 == 1)
        def _():
            down()
            for here in _cuts(s, sub):
                turn(here, t_s[here, :])
            gate_up_()

        @pl.when(at == tiles - 1)
        def _():
            for here in _cuts(s, sub):
                turn(here, _nt(y_ref[here, :], w_ref[:bn, :]).astype(BF16))
            down()
            gate_up_()

    return _call(
        body, (ff // bn,), [((s, d), _FLAT), ((2 * bn, d), lambda i: (i // 2, 0)), ((s, bn), _col), ((s, bn), _col), ((s, bn), _col), ((s, d), _FLAT)],
        [((s, bn), _col), ((s, bn), _col), ((bn, d), _row), ((n, 1, 2, rows, bn), lambda i: (0, i // per, 0, 0, i % per))],
        [_shape((s, ff)), _shape((s, ff)), _shape((ff, d)), _shape((n, 3, 2, rows, third))], 4 * s * d * ff, (y, w, g, u, act, b), [pltpu.VMEM((s, bn), BF16)],
    )


def after(*values):
    return lax.optimization_barrier(values)


def _tables(tokens):
    half = HEAD // 2
    place = np.arange(max(tokens, half), dtype=np.float32)
    angle = place[:tokens, None] * np.float32(THETA) ** (-place[:half] / np.float32(half))
    c, s = (f(angle.astype(np.float64)).astype(np.float32) for f in (np.cos, np.sin))
    return jnp.asarray(np.concatenate([c, c], -1)), jnp.asarray(np.concatenate([-s, s], -1))


def back_project_and_sum(a, d, g_out, w, h, by_h):
    (_, s, width), dim = d.shape, h.shape[1]
    n, _, rows, _ = w.shape
    bn, bm = 256, 256
    tiles = width // bn
    makes, backs = 3 * tiles, s // bm
    waves = 4

    def body(d_col, a_ref, d_row, h_ref, y_ref, w_hbm, go_hbm, o_ref, sum_ref, w_s, g_s, r0_s, *rest):
        a_s, s1, r1, s2, r2, s3, r3 = (rest[3 * i : 3 * i + 3] for i in range(7))
        w_sem, go_sem, send, recv, core_send, core_recv = rest[21:]
        t = _step()
        bits, core, other, across = _here()

        def at(dims, first, second, third):
            place = [None] * 3
            for dim_, number in zip(dims, (first, second, third)):
                place[dim_] = number
            return tuple(place)

        slot = (1, 0, 1, 0)

        def to_core(wave):
            source = g_s.at[slot[wave], :, :, :, 1 - core] if wave else go_hbm.at[:, :, :, 1 - core]
            return _send(source, r0_s.at[wave], core_send.at[wave], core_recv.at[wave], other)

        def hop(wave, k, stage):
            source, target = ((s1, r1), (s2, r2), (s3, r3))[stage]
            return _send(source[k].at[wave], target[k].at[wave], send.at[wave, stage, k], recv.at[wave, stage, k], across[_order(wave, k)[stage]])

        def mine_of_out():
            return pltpu.make_async_copy(go_hbm.at[:, :, :, core], g_s.at[1, :, :, :, core], go_sem)

        def weights():
            return pltpu.make_async_copy(w_hbm.at[:, pl.ds(0, 3)], w_s, w_sem)

        def add0(wave):
            to_core(wave).wait()
            if wave == 0:
                mine_of_out().wait()
            for k, part in enumerate(PARTS):
                dims = _order(wave, k)
                b = bits[dims[0]]

                def pair(i):
                    second, third = i // 2, i % 2

                    def total(first):
                        p = at(dims, first, second, third)
                        return g_s[(slot[wave], *p, core, ALL, part)].astype(F32) + r0_s[(wave, *p, ALL, part)].astype(F32)

                    s1[k][wave, second, third] = total(1 - b).astype(BF16)
                    a_s[k][wave, second, third] = total(b)

                _loop(4, pair)
            for k in WAYS:
                hop(wave, k, 0).start()

        def add1(wave):
            for k in WAYS:
                hop(wave, k, 0).wait_recv()
                b = bits[_order(wave, k)[1]]

                def one(third):
                    s2[k][wave, third] = (a_s[k][wave, 1 - b, third] + r1[k][wave, 1 - b, third].astype(F32)).astype(BF16)
                    a_s[k][wave, b, third] = a_s[k][wave, b, third] + r1[k][wave, b, third].astype(F32)

                _loop(2, one)
            for k in WAYS:
                hop(wave, k, 1).start()

        def add2(wave):
            for k in WAYS:
                hop(wave, k, 1).wait_recv()
                dims = _order(wave, k)
                b, c = bits[dims[1]], bits[dims[2]]
                s3[k][wave] = (a_s[k][wave, b, 1 - c] + r2[k][wave, 1 - c].astype(F32)).astype(BF16)
                a_s[k][wave, b, c] = a_s[k][wave, b, c] + r2[k][wave, c].astype(F32)
            for k in WAYS:
                hop(wave, k, 2).start()

        def add3(wave):
            for k, part in enumerate(PARTS):
                hop(wave, k, 2).wait_recv()
                dims = _order(wave, k)
                b, c = bits[dims[1]], bits[dims[2]]
                sum_ref[(wave + len(WAYS)) % waves, :, part] = (a_s[k][wave, b, c] + r3[k][wave].astype(F32)).astype(BF16)

        @pl.when(t == 0)
        def _():
            _meet((other, *across))
            to_core(0).start()
            mine_of_out().start()
            weights().start()

        @pl.when(t < makes)
        def _():
            made = _tn(a_ref[:], d_col[0]).astype(BF16).reshape(*TORUS, rows, bn)
            g_s[(t // tiles) % 2, :, :, :, :, :, pl.ds(pl.multiple_of(t % tiles * bn, bn), bn)] = made

        @pl.when(t == makes)
        def _():
            weights().wait()

        @pl.when(t >= makes)
        def _():
            part = sum(_nt(d_row[m], w_s[:, m].reshape(dim, width)) for m in range(3))
            o_ref[:] = _through_norm(h_ref[:], part, y_ref[:])

        last = makes + backs - 1
        plan = {add0: (3, 9, 14, 16), add1: (12, 18, 18, 19), add2: (16, 20, 20, 21), add3: (18, last, last, last)}
        for action, times in plan.items():
            for wave, step in enumerate(times):
                pl.when(t == step)(functools.partial(action, wave))
        for wave in range(1, waves):
            pl.when(t == tiles * wave - 1)(functools.partial(lambda i: to_core(i).start(), wave))

        @pl.when(t == last)
        def _():
            for wave in range(waves):
                for stage in WAYS:
                    for k in WAYS:
                        hop(wave, k, stage).wait_send()

    def made(t):
        return jnp.minimum(t, makes - 1)

    def back(t):
        return jnp.maximum(t - makes, 0)

    wide = [part.stop - part.start for part in PARTS]
    tile = lambda t: (back(t), 0)
    total, summed = pl.pallas_call(
        body,
        grid=(makes + backs,),
        in_specs=[
            pl.BlockSpec((1, s, bn), lambda t: (made(t) // tiles, 0, made(t) % tiles)), _spec((s, dim), _FLAT),
            pl.BlockSpec((3, bm, width), lambda t: (0, back(t), 0)), pl.BlockSpec((bm, dim), tile), pl.BlockSpec((bm, dim), tile),
            ANY, ANY,
        ],
        out_specs=[pl.BlockSpec((bm, dim), tile), pl.BlockSpec((waves, rows, width), _CUBE)],
        out_shape=[_shape((s, dim)), _shape((waves, rows, width))],
        scratch_shapes=[
            pltpu.VMEM((n, 3, rows, width), BF16), pltpu.VMEM((2, *TORUS, rows, width), BF16), pltpu.VMEM((waves, *TORUS[1:], rows, width), BF16),
            *(pltpu.VMEM((waves, 2, 2, rows, x), F32) for x in wide),
            *(pltpu.VMEM((waves, *((2,) * (2 - i)), rows, x), BF16) for i in WAYS for _ in range(2) for x in wide),
            pltpu.SemaphoreType.DMA, pltpu.SemaphoreType.DMA, *_link_sems(waves),
        ],
        compiler_params=pltpu.CompilerParams(vmem_limit_bytes=VMEM, dimension_semantics=("arbitrary",), collective_id=0, has_side_effects=True),
        cost_estimate=pl.CostEstimate(flops=12 * s * dim * width, bytes_accessed=60 * 2**20, transcendentals=0),
    )(d, a, d, h, by_h, w, g_out.reshape(*TORUS, rows, width))
    return total, summed


def collect(y, qkvo, gu, dn):
    layers, (s, d), (_, _, rows, third) = len(dn), y.shape, gu[0].shape
    ff = len(WAYS) * third
    shapes = [_shape(y.shape), *[_shape((layers, rows, d))] * 4, *[_shape((layers, rows, ff))] * 2, _shape((layers, *dn[0].shape))]
    parts = [y, *qkvo, *gu, *dn]

    def moves(l):
        if l < 0:
            return [(0, (here,), 0, (here,)) for here in _cuts(s, 512)]
        at = range(l + 1, len(parts), layers)
        return [
            *((at[0], (here,), i + 1, (l,)) for i, here in enumerate(_cuts(4 * rows, rows))),
            *((at[1], (k, i), 5 + i, (l, ALL, here)) for i in PAIR for k, here in enumerate(_cuts(ff, third))),
            (at[2], (), 7, (l,)),
        ]

    plan = [move for l in range(-1, layers) for move in moves(l)]

    def body(*refs):
        from_, to, held, came, left = refs[: len(parts)], refs[len(parts) :][: len(shapes)], refs[len(parts) + len(shapes) : -2], refs[-2], refs[-1]

        def bring(i):
            part, place, _, _ = plan[i]
            return pltpu.make_async_copy(from_[part].at[place], held[part].at[place], came.at[i])

        def put(i):
            part, place, out, target = plan[i]
            return pltpu.make_async_copy(held[part].at[place], to[out].at[target], left.at[i])

        for i in range(len(plan)):
            bring(i).start()
        for i in range(len(plan)):
            bring(i).wait()
            put(i).start()
        for i in range(len(plan)):
            put(i).wait()

    sems = [pltpu.SemaphoreType.DMA((len(plan),))] * 2
    any_ = (None, None)
    return _call(body, (1,), [any_] * len(parts), [any_] * len(shapes), shapes, s, parts, [*(pltpu.VMEM(x.shape, BF16) for x in parts), *sems])


def solution(mesh):
    n = mesh.shape["dp"]

    def gather(t):
        return lax.all_gather(t, "dp", tiled=True)

    def scatter(t):
        flat = lax.psum_scatter(t.reshape(-1, t.shape[-1]), "dp", tiled=True)
        return flat.reshape(t.shape[1:])

    def step(x, dy, wq, wk, wv, wo, w_gate, w_up, w_down):
        layers, rows, width = wq.shape
        ff = w_gate.shape[2]
        s = x.shape[1]
        cos, sin = _tables(s)
        h = x[0]
        kept = []
        for l in range(layers):
            if l:
                w_qkvo, w_gu = (gather(x).reshape(n, -1, rows, x.shape[-1]) for x in packed)
                w_out, w_dn = w_qkvo, gather(w_down[l])
                qkv = project(a, w_qkvo, cos, sin)
            else:
                w_out = gather(wo[l]).reshape(n, -1, rows, width)
                w_gu = gather(jnp.concatenate([w_gate[l], w_up[l]])).reshape(n, -1, rows, ff)
                a, qkv, w_qkvo, packed = fetch_and_project(h, cos, sin, (wq, wk, wv), ((wq, wk, wv, wo), (w_gate, w_up)))
            out, lse = attend(qkv)
            mid, b = add_matmul(out, w_out, h, (n, 1, rows, width), (0, w_out.shape[1] - 1, 0, 0))
            g, u, act, *carried = gate_up(b, w_gu, None if l else _Carry(w_down, 2, 56))
            w_dn = w_dn if l else carried[0].reshape(-1, w_down.shape[-1])
            kept.append((w_qkvo, w_out, w_gu, w_dn, h, a, qkv, out, lse, mid, b, g, u, act))
            if l + 1 < layers:
                h, a = add_matmul(act, w_dn, mid)

        y = dy[0]
        of = []
        for l in reversed(range(layers)):
            w_qkvo, w_out, w_gu, w_dn, h, a, qkv, out, lse, mid, b, g, u, act = kept[l]
            dg, du, g_dn, g_gu = mlp_back(y, w_dn, g, u, act, b, n)
            of_gu = scatter(g_gu)
            of_dn = scatter(g_dn.reshape(n, -1, g_dn.shape[1]))
            y_mid = back_gate_up(dg, du, w_gu, mid, y)
            if l == 0:
                g_out, y_mid = after(grad_out(out, y_mid, n), y_mid)
            d = attend_back(qkv, out, lse, y_mid, w_out, cos, sin)
            if l == 0:
                y, of_qkvo = back_project_and_sum(a, d, g_out, w_qkvo, h, y_mid)
                of.append((of_qkvo.reshape(-1, width), of_gu, of_dn))
                break
            g_qkvo, d = after(grad_project(a, d, out, y_mid, n), d)
            of_qkvo = scatter(g_qkvo)
            y = back_project(d, w_qkvo, h, y_mid)
            of.append((of_qkvo, of_gu, of_dn))
        y, *rest = collect(y, *zip(*reversed(of)))
        return y[None], *rest

    states, cut = P(("rep", "dp"), None, None), P(None, "dp", None)
    return jax.shard_map(
        step,
        mesh=mesh,
        in_specs=(states, states) + (cut,) * 7,
        out_specs=(states,) + (P("rep", "dp", None),) * 7,
        check_vma=False,
    )
```
